32 devices in a mesh: dp: 8 (over z, x), ctx: 4 (over y, core).
Axes of the slice: x: 2, y: 2, z: 4, core: 2. Of those that a mesh axis runs over, the one named last changes fastest.
Arguments:
- queries: bfloat16 [8, 1024, 2048], P('dp', 'ctx'), may hold values from -100 to 100
- keys: bfloat16 [8, 1024, 512], P('dp', 'ctx'), may hold values from -4 to 4
- values: bfloat16 [8, 1024, 512], P('dp', 'ctx'), may hold values from -6 to 6
- segments: int32 [8, 1024], P('dp', 'ctx'), may hold values from 0 to 7, never falling along the last dimension, each value on 1 to 512 neighbouring positions
Outputs:
- attended: bfloat16 [8, 1024, 2048], P('dp', 'ctx')
The draws below stay inside these ranges and needn't reach their ends.
Inputs may be any that keep to these rules, and one draw needn't show every extreme that they name: `segments`: document numbers never fall along a packed batch, every one of the 8 documents is present, and each document has at most 512 tokens; some document has exactly 512.
All inputs are finite; a program needn't handle non-finite values.
Results may differ from the reference program's by a relative error of at most 0.0053.
Values may be sent and summed in bfloat16 or wider, within the bound.
A program may use at most 192 MiB of HBM per device.

```python
import math
import jax
import jax.numpy as jnp
import numpy as np
from jax import lax

HQ = 16
HK = 4
HD = 128
SEQ_COUNT = 8
TOKENS = 1024
MOST = 512
N_DP = 8


def draw_pair(key):
    key_keys = jax.random.fold_in(key, 12)
    key_queries = jax.random.fold_in(key, 11)
    key_rows = jnp.clip(jax.random.normal(key_keys, (N_DP, TOKENS, HK * HD), jnp.float32), -4.0, 4.0)
    query_rows = jnp.clip(jax.random.normal(key_queries, (N_DP, TOKENS, HQ * HD), jnp.float32), -4.0, 4.0)
    return (query_rows, key_rows)


def draw_queries(key, part):
    return draw_pair(key)[0].astype(jnp.bfloat16)


def draw_keys(key, part):
    return draw_pair(key)[1].astype(jnp.bfloat16)


def level_of(rng, shape, cuts, smallest, largest):
    factor_of = 1.0
    for dim, blocks in cuts:
        draws = jax.random.uniform(jax.random.fold_in(jax.random.fold_in(rng, 6), dim), (blocks,), jnp.float32, smallest / len(cuts), largest / len(cuts))
        factor_of = factor_of * jnp.repeat(jnp.exp(draws), shape[dim] // blocks).reshape((-1,) + (1,) * (len(shape) - 1 - dim))
    return factor_of


def length_profile(number_of, total, bound, skew):
    loads = [(1 << 20) // math.isqrt(grade ** skew) + 1 for grade in range(2, number_of + 1)]
    spare, counts = total - bound - (number_of - 1), [1] * (number_of - 1)
    while spare > 0:
        movable = [i for i in range(number_of - 1) if counts[i] < bound]
        whole, left = sum([loads[i] for i in movable]), spare
        for i in movable:
            addition = min(bound - counts[i], max(1, left * loads[i] // whole), spare)
            counts[i] = counts[i] + addition
            spare = spare - addition
    return np.array([bound] + counts)


def ragged(own_key, number_of, total, reach, skew):
    if number_of == 2:
        one = jax.random.randint(own_key, (), max(1, total - reach), min(reach, total - 1) + 1)
        return jnp.stack([one, total - one])
    sizes = jnp.asarray(length_profile(number_of, total, reach, skew), jnp.int32)
    pairs = (number_of - 1) // 2
    giver, receiver = sizes[1:1 + 2 * pairs:2], sizes[2:2 + 2 * pairs:2]
    slack = jnp.minimum(giver - 1, reach - receiver)
    moved = jax.random.randint(jax.random.fold_in(own_key, 1), (pairs,), 0, 1 << 20) % (slack + 1)
    sizes = sizes.at[1:1 + 2 * pairs:2].set(giver - moved).at[2:2 + 2 * pairs:2].set(receiver + moved)
    return sizes[jax.random.permutation(jax.random.fold_in(own_key, 2), number_of)]


def scatter_about(stream_key, extent, scale, bound, cuts=(), held_as=jnp.bfloat16):
    entries = jax.random.normal(stream_key, extent, jnp.float32) * scale
    if len(cuts) > 0:
        entries = level_of(stream_key, extent, cuts, -0.22, 0.18) * entries
    return jnp.clip(entries, min=-bound, max=bound).astype(held_as)


def setup_inputs(seed: int = 0) -> dict:
    streams_of = jax.random.split(jax.random.key(seed), 5)
    queries = draw_queries(jax.random.fold_in(streams_of[4], 71), 0)
    keys = draw_keys(jax.random.fold_in(streams_of[4], 71), 0)
    values = scatter_about(streams_of[2], (N_DP, TOKENS, HK * HD), 1.0, 6.0, ((0, 8), (1, 4)))
    segments = jax.vmap(lambda own: jnp.searchsorted(jnp.cumsum(ragged(own, SEQ_COUNT, TOKENS, MOST, 2)), jnp.arange(TOKENS), side="right"))(jax.random.split(streams_of[3], N_DP)).reshape((N_DP, TOKENS)).astype(jnp.int32)
    return dict(queries=queries, keys=keys, values=values, segments=segments)


rope_theta = 500000.0

def rotate(values_in, positions, heads):
    rows = values_in.shape[0]
    half_dim = HD // 2
    split = values_in.astype(jnp.float32).reshape(rows, heads, HD)
    inv_freq = jnp.exp(-jnp.log(rope_theta) * 2.0 * jnp.arange(half_dim, dtype=jnp.float32) / HD)
    angles = positions.astype(jnp.float32)[:, None] * inv_freq[None, :]
    cosine_part = jnp.cos(angles)[:, None, :]
    sine_part = jnp.sin(angles)[:, None, :]
    first_half = split[..., :half_dim]
    second_half = split[..., half_dim:]
    turned = jnp.concatenate([first_half * cosine_part - second_half * sine_part, second_half * cosine_part + first_half * sine_part], axis=-1)
    return turned.reshape(rows, heads * HD).astype(jnp.bfloat16)

def doc_positions(seg_ids):
    index_all = jnp.arange(seg_ids.shape[0], dtype=jnp.int32)
    previous = jnp.concatenate([seg_ids[:1] - 1, seg_ids[:-1]])
    run_start = lax.cummax(jnp.where(seg_ids != previous, index_all, 0), axis=0)
    return index_all - run_start

def one_batch(inputs):
    query_rows, key_rows, value_rows, seg_ids = inputs
    positions = doc_positions(seg_ids)
    rot_q = rotate(query_rows, positions, HQ)
    rot_k = rotate(key_rows, positions, HK)
    block_rows = min(512, TOKENS)
    pieces = []
    for block_index in range(TOKENS // block_rows):
        q_lo = block_index * block_rows
        key_lo = max(0, q_lo - MOST)
        key_hi = q_lo + block_rows
        width = key_hi - key_lo
        query_heads = rot_q[q_lo:key_hi].astype(jnp.float32).reshape(block_rows, HK, HQ // HK, HD)
        key_heads = rot_k[key_lo:key_hi].astype(jnp.float32).reshape(width, HK, HD)
        value_heads = value_rows[key_lo:key_hi].astype(jnp.float32).reshape(width, HK, HD)
        q_index = q_lo + jnp.arange(block_rows, dtype=jnp.int32)
        k_index = key_lo + jnp.arange(width, dtype=jnp.int32)
        live_mask = (seg_ids[key_lo:key_hi][None, :] == seg_ids[q_lo:key_hi][:, None]) & (k_index[None, :] <= q_index[:, None])
        scores = jnp.einsum('thgd,shd->hgts', query_heads, key_heads) / jnp.sqrt(jnp.float32(HD))
        scores = jnp.where(live_mask, scores, jnp.float32(-1e+30))
        row_max = lax.optimization_barrier(jnp.max(scores, axis=-1, keepdims=True))
        weights = jnp.where(live_mask, jnp.exp(scores - row_max), jnp.float32(0.0))
        denom = lax.optimization_barrier(jnp.sum(weights, axis=-1))
        rounded = lax.optimization_barrier(weights.astype(jnp.bfloat16)).astype(jnp.float32)
        weighted = jnp.einsum('hgts,shd->thgd', rounded, value_heads)
        result = weighted / jnp.transpose(denom, (2, 0, 1))[..., None]
        pieces.append(result.reshape(block_rows, HQ * HD).astype(jnp.bfloat16))
    return jnp.concatenate(pieces, axis=0)

def reference(queries, keys, values, segments):
    attended = lax.map(one_batch, (queries, keys, values, segments))
    return attended
```

```python
import functools
import math

import jax
import jax.numpy as jnp
from jax import lax
from jax.experimental import pallas as pl
from jax.experimental.pallas import tpu as pltpu
from jax.sharding import PartitionSpec as P

HK = 4
HD = 128
THETA = 500000.0
LANES = 128
MASKED = -1e30
F32 = jnp.float32
BF16 = jnp.bfloat16


def sin_cos(angle):
    turns = jnp.floor(angle * (2.0 / math.pi) + 0.5)
    rest = angle - turns * 1.5703125
    rest = rest - turns * 4.837512969970703125e-4
    rest = rest - turns * 7.54978995489188216e-8
    square = rest * rest
    sine = rest + rest * square * (
        -1.6666654611e-1 + square * (8.3321608736e-3 + square * -1.9515295891e-4)
    )
    cosine = (
        1.0
        - 0.5 * square
        + square * square * (4.166664568298827e-2 + square * (-1.388731625493765e-3 + square * 2.443315711809948e-5))
    )
    quarter = turns - 4.0 * jnp.floor(turns * 0.25)
    odd = (quarter == 1.0) | (quarter == 3.0)
    sin_out = jnp.where(odd, cosine, sine)
    cos_out = jnp.where(odd, sine, cosine)
    sin_out = jnp.where(quarter >= 2.0, -sin_out, sin_out)
    cos_out = jnp.where((quarter == 1.0) | (quarter == 2.0), -cos_out, cos_out)
    return sin_out, cos_out


def frequencies():
    index = lax.broadcasted_iota(jnp.int32, (1, HD), 1) % (HD // 2)
    result = jnp.ones((1, HD), F32)
    bit = 1
    while bit < HD // 2:
        factor = math.exp(-math.log(THETA) * 2.0 * bit / HD)
        result = result * jnp.where((index // bit) % 2 == 1, F32(factor), F32(1.0))
        bit *= 2
    return result


def turned(block, cosine, sine):
    block = block.astype(F32)
    return (block * cosine + pltpu.roll(block, HD // 2, 1) * sine).astype(BF16)


def kernel(
    count, hops, q_ref, k_ref, v_ref, seg_ref, out_ref,
    q_own, kwin, vwin, segwin, krot, qrot, weights, denoms, sines, cosines, bias,
    q_sem, seg_sem, own_sem, seg_send, seg_recv, send, recv, forward,
):
    me = lax.axis_index("ctx")
    rows = q_own.shape[0]
    span = bias.shape[2]
    group = qrot.shape[0] // HK
    windows = (kwin, vwin)

    def block(which, head, distance):
        return windows[which].at[head, pl.ds((hops - distance) * rows, rows)]

    own_copies = [
        [
            pltpu.make_async_copy(
                ref.at[0, :, pl.ds(head * HD, HD)], block(which, head, 0), own_sem.at[which, head]
            )
            for head in range(HK)
        ]
        for which, ref in enumerate((k_ref, v_ref))
    ]
    seg_copy = pltpu.make_async_copy(seg_ref, segwin.at[hops], seg_sem)
    q_copy = pltpu.make_async_copy(q_ref.at[0], q_own, q_sem)
    seg_copy.start()
    for which in range(2):
        for head in range(HK):
            own_copies[which][head].start()
    q_copy.start()

    barrier = pltpu.get_barrier_semaphore()
    for distance in range(1, hops + 1):
        @pl.when(me + distance < count)
        def _():
            pl.semaphore_signal(barrier, inc=1, device_id={"ctx": me + distance})

        @pl.when(me >= distance)
        def _():
            pl.semaphore_signal(barrier, inc=1, device_id={"ctx": me - distance})
    pl.semaphore_wait(barrier, jnp.minimum(me, hops) + jnp.minimum(count - 1 - me, hops))

    def seg_out(distance):
        return pltpu.make_async_remote_copy(
            src_ref=segwin.at[hops], dst_ref=segwin.at[hops - distance],
            send_sem=seg_send.at[distance - 1], recv_sem=seg_recv.at[distance - 1],
            device_id={"ctx": me + distance},
        )

    def block_out(which, head, distance):
        return pltpu.make_async_remote_copy(
            src_ref=block(which, head, 0), dst_ref=block(which, head, distance),
            send_sem=send.at[which, head, distance - 1], recv_sem=recv.at[which, head, distance - 1],
            device_id={"ctx": me + distance},
        )

    def block_on(which, head, distance):
        return pltpu.make_async_remote_copy(
            src_ref=block(which, head, distance), dst_ref=block(which, head, distance + 1),
            send_sem=forward.at[which, head, distance - 1], recv_sem=recv.at[which, head, distance],
            device_id={"ctx": me + 1},
        )

    def goes_out(distance):
        direct = me + distance < count
        if distance > 1:
            direct = direct & ((me + distance) % 2 == 0)
        return direct

    def goes_on(distance):
        return (me % 2 == 0) & (me >= distance) & (me + 1 < count)

    seg_copy.wait()
    for distance in range(1, hops + 1):
        @pl.when(me + distance < count)
        def _():
            seg_out(distance).start()
    for which in range(2):
        for head in range(HK):
            own_copies[which][head].wait()

            @pl.when(goes_out(1))
            def _():
                block_out(which, head, 1).start()
    for distance in range(2, hops + 1):
        @pl.when(goes_out(distance))
        def _():
            for which in range(2):
                for head in range(HK):
                    if distance == 2:
                        block_out(which, head, 1).wait_send()
                    block_out(which, head, distance).start()

    for distance in range(1, hops + 1):
        @pl.when(me < distance)
        def _():
            empty = jnp.zeros((HK, rows, HD), BF16)
            kwin[:, pl.ds((hops - distance) * rows, rows)] = empty
            vwin[:, pl.ds((hops - distance) * rows, rows)] = empty
            segwin[hops - distance] = jnp.full((1, rows), -1, jnp.int32)

    for distance in range(1, hops + 1):
        @pl.when(me >= distance)
        def _():
            seg_out(distance).wait_recv()

    freq = frequencies()
    lane = lax.broadcasted_iota(jnp.int32, (rows, LANES), 1)
    row = lax.broadcasted_iota(jnp.int32, (rows, LANES), 0)
    sign = jnp.where(lane < HD // 2, F32(-1.0), F32(1.0))
    ones = jnp.ones((LANES, LANES), BF16)
    pieces = []
    for index in range(hops + 1):
        seg_row = segwin[index].astype(F32)
        pieces += [seg_row[:, at:at + LANES] for at in range(0, rows, LANES)]
    for index in range(hops + 1):
        column = jnp.broadcast_to(segwin[index].astype(F32), (LANES, rows)).T
        smaller = jnp.zeros((rows, LANES), F32)
        for piece in pieces:
            smaller = smaller + jnp.where(piece < column, F32(1.0), F32(0.0))
        start = jnp.dot(smaller.astype(BF16), ones, preferred_element_type=F32)
        position = (row + index * rows).astype(F32) - start
        sine, cosine = sin_cos(position * freq)
        sines[index] = sine * sign
        cosines[index] = cosine
        if index == hops:
            last = (row + hops * rows).astype(F32)
            for tile in range(rows // LANES):
                mine = slice(tile * LANES, (tile + 1) * LANES)
                for at in range(0, span, LANES):
                    spot = (lane[mine] + (at + tile * LANES)).astype(F32)
                    bias[tile, :, at:at + LANES] = jnp.where(
                        (spot >= start[mine]) & (spot <= last[mine]), F32(0.0), F32(MASKED)
                    )

    q_copy.wait()

    @pl.loop(0, qrot.shape[0])
    def _(head):
        at = pl.ds(pl.multiple_of(head * HD, HD), HD)
        qrot[head] = turned(q_own[:, at], cosines[hops], sines[hops])

    scale = F32(math.log2(math.e) / math.sqrt(HD))

    def arrive(head, distance, which):
        @pl.when(me >= distance)
        def _():
            block_out(which, head, distance).wait_recv()
        if distance < hops:
            @pl.when(goes_on(distance))
            def _():
                block_on(which, head, distance).start()

    @pl.loop(0, HK)
    def _(head):
        for distance in range(1, hops + 1):
            arrive(head, distance, 0)
        for index in range(hops + 1):
            at = pl.ds(index * rows, rows)
            krot[at] = turned(kwin[head, at], cosines[index], sines[index])

        for part in range(group):
            for tile in range(rows // LANES):
                mine = slice(tile * LANES, (tile + 1) * LANES)
                seen = pl.ds(tile * LANES, span)
                scores = lax.dot_general(
                    qrot[head * group + part, mine], krot[seen], (((1,), (1,)), ((), ())),
                    preferred_element_type=F32,
                ) + bias[tile]
                top = jnp.max(scores, axis=1, keepdims=True)
                weight = jnp.exp2((scores - top) * scale)
                denoms[head * group + part, mine] = jnp.broadcast_to(
                    jnp.sum(weight, axis=1, keepdims=True), (LANES, LANES)
                )
                weights[head * group + part, mine] = weight.astype(BF16)

    for distance in range(1, hops):
        arrive(0, distance, 1)

    @pl.loop(0, HK)
    def _(head):
        @pl.when(head + 1 < HK)
        def _():
            for distance in range(1, hops):
                arrive(head + 1, distance, 1)

        arrive(head, hops, 1)

        for part in range(group):
            for tile in range(rows // LANES):
                mine = slice(tile * LANES, (tile + 1) * LANES)
                seen = pl.ds(tile * LANES, span)
                total = jnp.dot(weights[head * group + part, mine], vwin[head, seen], preferred_element_type=F32)
                at = pl.ds(pl.multiple_of((head * group + part) * HD, HD), HD)
                out_ref[0, mine, at] = (total / denoms[head * group + part, mine]).astype(BF16)

    for distance in range(1, hops + 1):
        @pl.when(me + distance < count)
        def _():
            seg_out(distance).wait_send()
        unsent = goes_out(distance)
        if distance == 1 and hops > 1:
            unsent = unsent & jnp.logical_not(goes_out(2))
        for which in range(2):
            for head in range(HK):
                @pl.when(unsent)
                def _():
                    block_out(which, head, distance).wait_send()
                if distance < hops:
                    @pl.when(goes_on(distance))
                    def _():
                        block_on(which, head, distance).wait_send()


def relay_kernel(
    q_ref, k_ref, v_ref, seg_ref, out_ref,
    q_own, win, segwin, krot, vturn, qrot, tops, totals, sines, cosines, bias,
    q_in, mix, lse_out, lse_in, q_sine, q_cosine, q_bias, mark, q_next, next_rot, next_bias, next_out,
    q_sem, seg_sem, own_sem, seg_send, seg_recv, back_send, back_recv, own_send, own_recv,
    near_send, near_recv, mix_send, mix_recv, lse_send, lse_recv, q_send, q_recv,
    help_send, help_recv, give_send, give_recv,
):
    me = lax.axis_index("ctx")
    count = lax.axis_size("ctx")
    rows = q_own.shape[0]
    heads = q_in.shape[0]
    group = heads // HK
    scale = F32(math.log2(math.e) / math.sqrt(HD))

    def blocks(first, last):
        if isinstance(first, int):
            return pl.ds(first * LANES, (last - first) * LANES)
        return pl.ds(pl.multiple_of(first * LANES, LANES), LANES)

    def columns(head):
        return pl.ds(head * HD if isinstance(head, int) else pl.multiple_of(head * HD, HD), HD)

    every = [(which, head) for head in range(HK) for which in range(2)]
    own_copies = {
        (which, head, tile): pltpu.make_async_copy(
            (k_ref, v_ref)[which].at[0, blocks(tile, tile + 1), columns(head)],
            win.at[which, head, blocks(4 + tile, 5 + tile)], own_sem.at[which, head, tile],
        )
        for which, head in every
        for tile in range(2)
    }
    seg_copy = pltpu.make_async_copy(seg_ref, segwin.at[2], seg_sem)
    q_copies = [
        pltpu.make_async_copy(
            q_ref.at[0, blocks(tile, tile + 1)], q_own.at[blocks(tile, tile + 1)], q_sem.at[tile]
        )
        for tile in range(2)
    ]
    tail = pl.ds((HK - 1) * group * HD, group * HD)
    keep_copy = pltpu.make_async_copy(q_ref.at[0, :, tail], q_own.at[:, tail], q_sem.at[0])
    seg_copy.start()

    barrier = pltpu.get_barrier_semaphore()

    def greet(step, here):
        @pl.when(here)
        def _():
            pl.semaphore_signal(barrier, inc=1, device_id={"ctx": me + step})

    greet(1, me + 1 < count)
    greet(-1, me >= 1)
    greet(2, me + 2 < count)
    greet(-2, me >= 2)

    pl.semaphore_wait(barrier, jnp.minimum(me, 2) + jnp.minimum(count - 1 - me, 2))

    def remote(source, target, sent, received, there):
        return pltpu.make_async_remote_copy(
            src_ref=source, dst_ref=target, send_sem=sent, recv_sem=received, device_id={"ctx": there}
        )

    def seg_out(distance):
        return remote(
            segwin.at[2], segwin.at[2 - distance], seg_send.at[distance - 1], seg_recv.at[distance - 1], me + distance
        )

    def seg_back():
        return remote(segwin.at[2], segwin.at[1], seg_send.at[2], seg_recv.at[2], me - 1)

    def own_out(which, head):
        return remote(
            (k_ref, v_ref)[which].at[0, :, columns(head)], win.at[which, head, blocks(2, 4)],
            own_send.at[which, head], own_recv.at[which, head], me + 1,
        )

    def own_back(which, head):
        return remote(
            (k_ref, v_ref)[which].at[0, :, columns(head)], win.at[which, head, blocks(6, 8)],
            back_send.at[which, head], back_recv.at[which, head], me - 1,
        )

    def help_out(head):
        at = pl.ds(head * group * HD, group * HD)
        return remote(q_ref.at[0, :, at], q_next.at[:, at], help_send.at[head], help_recv.at[head], me - 1)

    def give_out(head):
        width = group * HD
        at = pl.ds(head * width if isinstance(head, int) else pl.multiple_of(head * width, width), width)
        return remote(next_out.at[:, at], out_ref.at[0, :, at], give_send.at[head], give_recv.at[head], me + 1)

    def near_out(which, head):
        return remote(
            (k_ref, v_ref)[which].at[0, blocks(1, 2), columns(head)], win.at[which, head, blocks(3, 4)],
            near_send.at[which, head], near_recv.at[which, head], me + 1,
        )

    def near_on(which, head):
        return remote(
            win.at[which, head, blocks(3, 4)], win.at[which, head, blocks(1, 2)],
            near_send.at[which, head], near_recv.at[which, head], me + 1,
        )

    def spot(piece, base):
        at = pl.multiple_of((base - piece // (2 * HK)) * LANES, LANES)
        return (piece % 2, (piece % (2 * HK)) // 2, pl.ds(at, LANES))

    def mix_out(piece):
        return remote(mix.at[piece], win.at[spot(piece, 2)], mix_send.at[piece], mix_recv.at[piece], me + 1)

    def mix_on(which, head):
        piece = 2 * head + which
        return remote(
            win.at[which, head, blocks(2, 3)], win.at[which, head, blocks(0, 1)],
            mix_send.at[piece], mix_recv.at[piece], me + 1,
        )

    def lse_copy(pair):
        return remote(lse_out.at[pair], lse_in.at[pair], lse_send.at[pair], lse_recv.at[pair], me + 1)

    def q_back(which):
        return remote(
            q_ref.at[0, blocks(0, 1), columns(which)], q_in.at[which], q_send.at[which], q_recv.at[which], me - 1
        )

    freq = frequencies()
    lane = lax.broadcasted_iota(jnp.int32, (LANES, LANES), 1)
    row = lax.broadcasted_iota(jnp.int32, (LANES, LANES), 0)
    sign = jnp.where(lane < HD // 2, F32(-1.0), F32(1.0))
    ones = jnp.ones((LANES, LANES), BF16)

    def start_of(index, pieces):
        column = jnp.broadcast_to(segwin[index].astype(F32), (LANES, rows)).T
        smaller = jnp.zeros((rows, LANES), F32)
        for piece in pieces:
            smaller = smaller + jnp.where(piece < column, F32(1.0), F32(0.0))
        return jnp.dot(smaller.astype(BF16), ones, preferred_element_type=F32)

    def tables(start, block):
        sine, cosine = sin_cos(((row + block * LANES).astype(F32) - start) * freq)
        at = blocks(block, block + 1)
        sines[at] = sine * sign
        cosines[at] = cosine

    def masks(where, start, tile, low, own):
        first = start.T
        last = (lane + (own + tile) * LANES).astype(F32)
        for block in range(low, own + 1 + tile):
            key = (row + block * LANES).astype(F32)
            live = key >= first
            if block == own + tile:
                live = live & (key <= last)
            where[tile, blocks(block, block + 1)] = jnp.where(live, F32(0.0), F32(MASKED))

    def turn_key(head, block):
        at = blocks(block, block + 1)
        krot[head, at] = turned(win[0, head, at], cosines[at], sines[at])
        vturn[head, 0:HD, at] = win[1, head, at].T

    def turn_queries(head, source, target, own):
        for tile in range(2):
            place = blocks(own + tile, own + 1 + tile)
            cosine, sine = cosines[place], sines[place]
            for member in range(group):
                target[head, tile, blocks(member, member + 1)] = turned(
                    source[blocks(tile, tile + 1), columns(head * group + member)], cosine, sine
                )

    def raw_scores(keys, one):
        return lax.dot_general(keys, one, (((1,), (1,)), ((), ())), preferred_element_type=F32)

    def spread(part):
        return jnp.concatenate([part] * group, axis=1)

    def scores_of(head, tile, first, last):
        at = blocks(first, last)
        return raw_scores(krot[head, at], qrot[head, tile]) + spread(bias[tile, at])

    def summed(head, weight, at):
        return jnp.dot(vturn[head, :, at], weight.astype(BF16), preferred_element_type=F32)

    def keep(head, tile, top, both):
        tops[head, tile] = jnp.broadcast_to(top, tops.shape[2:])
        totals[head, tile] = both

    def put(head, tile, total, under, target=None):
        value = (total * (1.0 / under)).astype(BF16)
        for member in range(group):
            done = value[:, member * LANES:(member + 1) * LANES].T
            if target is None:
                out_ref[0, blocks(tile, tile + 1), columns(head * group + member)] = done
            else:
                target[blocks(tile, tile + 1), columns(head * group + member)] = done

    def fresh(head, first, last=5, ones=qrot, mask=bias):
        found = []
        for tile in range(2):
            at = blocks(first, last + tile)
            found.append(raw_scores(krot[head, at], ones[head, tile]) + spread(mask[tile, at]))
        result = []
        for tile in range(2):
            top = jnp.max(found[tile], axis=0, keepdims=True)
            weight = jnp.exp2((found[tile] - top) * scale)
            result.append((top, summed(head, weight, blocks(first, last + tile))))
        return result

    def more(head, tile, scores, first, last, extra=None):
        old = tops[head, tile, 0:1]
        top = jnp.maximum(old, jnp.max(scores, axis=0, keepdims=True))
        if extra is not None:
            top = jnp.maximum(top, extra)
        ratio = jnp.exp2((old - top) * scale)
        weight = jnp.exp2((scores - top) * scale)
        return top, totals[head, tile] * ratio + summed(head, weight, blocks(first, last))

    seg_copy.wait()
    for distance in (1, 2):
        @pl.when(me + distance < count)
        def _():
            seg_out(distance).start()

    @pl.when(me == 1)
    def _():
        seg_back().start()

    @pl.when(me == 2)
    def _():
        for which in range(heads):
            q_back(which).start()

    @pl.when(me == 1)
    def _():
        for which, head in every:
            near_out(which, head).start()
        for which, head in every[:-2]:
            own_back(which, head).start()
        for head in range(HK - 1):
            help_out(head).start()

    @pl.when(me % 2 == 0)
    def _():
        for which, head in every:
            own_out(which, head).start()

    for tile in (1, 0):
        for which, head in every:
            own_copies[which, head, tile].start()

    @pl.when(me == 1)
    def _():
        keep_copy.start()

    @pl.when(me != 1)
    def _():
        for tile in range(2):
            q_copies[tile].start()

    @pl.when(me <= 1)
    def _():
        segwin[0] = jnp.full((1, rows), -1, jnp.int32)

    @pl.when(me == 0)
    def _():
        seg_back().wait_recv()

    for distance in (1, 2):
        @pl.when(me >= distance)
        def _():
            seg_out(distance).wait_recv()

    for which, head in every:
        for tile in range(2):
            own_copies[which, head, tile].wait()

    pieces = []
    for index in range(3):
        seg_row = segwin[index].astype(F32)
        pieces += [seg_row[:, at:at + LANES] for at in range(0, rows, LANES)]
    shift = jnp.where(me == 0, rows, 0).astype(F32)
    begin = start_of(2, pieces) + shift
    start = start_of(1, pieces) + shift
    vturn[:, HD:] = jnp.ones((HK, vturn.shape[1] - HD, vturn.shape[2]), BF16)
    tables(begin[:LANES], 4)
    for tile in range(2):
        tables(start[tile * LANES:(tile + 1) * LANES], jnp.where(me == 0, 6, 2) + tile)

    @pl.when(me == 1)
    def _():
        late = begin[rows - 1:rows]
        sine, cosine = sin_cos(((row + 6 * LANES).astype(F32) - late) * freq)
        q_sine[...] = sine * sign
        q_cosine[...] = cosine
        for block in range(3):
            key = (row + (2 + block) * LANES).astype(F32)
            q_bias[blocks(block, block + 1)] = jnp.where(key >= late, F32(0.0), F32(MASKED))
        given = late < F32(3 * LANES)
        seen = blocks(2, 5)
        for head in range(HK):
            turn_key(head, 4)
        for which, head in every:
            own_out(which, head).wait_recv()

        @pl.loop(0, HK)
        def _(head):
            turn_key(head, 2)
            turn_key(head, 3)
            for pair in range(group // 2):
                twin = [head * group + 2 * pair + member for member in range(2)]
                for which in twin:
                    q_back(which).wait_recv()
                one = jnp.concatenate([turned(q_in[which], q_cosine[...], q_sine[...]) for which in twin], axis=0)
                scores = raw_scores(krot[head, seen], one) + jnp.concatenate([q_bias[...]] * 2, axis=1)
                top = jnp.max(scores, axis=0, keepdims=True)
                both = summed(head, jnp.exp2((scores - top) * scale), seen)
                under = both[HD:HD + 1]
                total = both[:HD] * (1.0 / under)
                for member, which in enumerate(twin):
                    mix[which] = jnp.where(
                        given, total[:, member * LANES:(member + 1) * LANES], win[spot(which, 4)].astype(F32)
                    ).astype(BF16)
                lse = top + jnp.log(under) * F32(math.sqrt(HD))
                for member in range(2):
                    lse_out[2 * head + pair, member:member + 1] = lse[:, member * LANES:(member + 1) * LANES]
                for which in twin:
                    mix_out(which).start()
                lse_copy(2 * head + pair).start()

    tables(begin[LANES:], 5)
    mark[...] = begin[:LANES].T[:8]
    first = jnp.where((begin < F32(LANES)) & (me == 2), F32(3 * LANES), begin)
    for tile in range(2):
        masks(bias, first[tile * LANES:(tile + 1) * LANES], tile, 0, 4)

    @pl.when(me == 1)
    def _():
        keep_copy.wait()
        head = HK - 1
        turn_queries(head, q_own, qrot, 4)
        turn_key(head, 5)
        for tile, (top, both) in enumerate(fresh(head, 2)):
            put(head, tile, both[:HD], both[HD:HD + 1])

    @pl.when(me == 0)
    def _():
        for tile in range(2):
            masks(next_bias, start[tile * LANES:(tile + 1) * LANES], tile, 4, 6)
            q_copies[tile].wait()

        @pl.loop(0, HK)
        def _(head):
            turn_queries(head, q_own, qrot, 4)
            for block in (4, 5):
                turn_key(head, block)
            for tile, (top, both) in enumerate(fresh(head, 4)):
                put(head, tile, both[:HD], both[HD:HD + 1])

        for which, head in every[:-2]:
            own_back(which, head).wait_recv()
        for head in range(HK - 1):
            help_out(head).wait_recv()

        @pl.loop(0, HK - 1)
        def _(head):
            turn_queries(head, q_next, next_rot, 6)
            for block in (6, 7):
                turn_key(head, block)
            for tile, (top, both) in enumerate(fresh(head, 4, 7, next_rot, next_bias)):
                put(head, tile, both[:HD], both[HD:HD + 1], next_out)
            give_out(head).start()

    @pl.when(me >= 2)
    def _():
        start = start_of(0, pieces)
        for tile in range(2):
            tables(start[tile * LANES:(tile + 1) * LANES], tile)

        for tile in range(2):
            q_copies[tile].wait()

        @pl.loop(0, HK)
        def _(head):
            turn_queries(head, q_own, qrot, 4)
            for block in (4, 5):
                turn_key(head, block)

    @pl.when(me == 2)
    def _():
        @pl.loop(0, HK)
        def _(head):
            for which in range(2):
                near_out(which, head).wait_recv()
                near_on(which, head).start()
            turn_key(head, 3)
            for tile, (top, both) in enumerate(fresh(head, 3)):
                keep(head, tile, top, both)

        @pl.loop(0, HK)
        def _(head):
            for which in range(2):
                mix_out(2 * head + which).wait_recv()
                mix_on(which, head).start()
            turn_key(head, 2)
            found = [scores_of(head, tile, 2, 3) for tile in range(2)]
            for tile in range(2):
                keep(head, tile, *more(head, tile, found[tile], 2, 3))

        @pl.loop(0, HK)
        def _(head):
            for which in range(2):
                mix_out(2 * HK + 2 * head + which).wait_recv()
                lse_copy(2 * head + which).wait_recv()
            turn_key(head, 1)
            found = [scores_of(head, tile, 1, 2) for tile in range(2)]
            crossing = spread(mark[0:1] < F32(LANES))
            lse = jnp.concatenate(
                [lse_in[2 * head + member // 2, member % 2:member % 2 + 1] for member in range(group)], axis=1
            )
            lse = jnp.where(crossing, lse, F32(MASKED))
            top, both = more(head, 0, found[0], 1, 2, lse)
            share = jnp.exp2((lse - top) * scale)
            given = jnp.concatenate([win[spot(head * group + member, 2)] for member in range(group)], axis=1)
            put(head, 0, both[:HD] + given.astype(F32) * share, both[HD:HD + 1] + share)
            top, both = more(head, 1, found[1], 1, 2)
            put(head, 1, both[:HD], both[HD:HD + 1])

    @pl.when(me == 3)
    def _():
        @pl.loop(0, HK)
        def _(head):
            for which in range(2):
                own_out(which, head).wait_recv()
            for block in (2, 3):
                turn_key(head, block)
            for tile, (top, both) in enumerate(fresh(head, 2)):
                keep(head, tile, top, both)

        @pl.loop(0, HK)
        def _(head):
            for which in range(2):
                near_on(which, head).wait_recv()
                mix_on(which, head).wait_recv()
            for block in range(2):
                turn_key(head, block)
            found = [scores_of(head, tile, tile, 2) for tile in range(2)]
            for tile in range(2):
                top, both = more(head, tile, found[tile], tile, 2)
                put(head, tile, both[:HD], both[HD:HD + 1])

    for distance in (1, 2):
        @pl.when(me + distance < count)
        def _():
            seg_out(distance).wait_send()

    @pl.when(me % 2 == 0)
    def _():
        for which, head in every:
            own_out(which, head).wait_send()

    @pl.when(me == 0)
    def _():
        for head in range(HK - 1):
            give_out(head).wait_send()

    @pl.when(me == 1)
    def _():
        @pl.loop(0, 2 * HK)
        def _(pair):
            for member in range(2):
                mix_out(2 * pair + member).wait_send()
            lse_copy(pair).wait_send()

        for head in range(HK - 1):
            help_out(head).wait_send()
            give_out(head).wait_recv()
        seg_back().wait_send()
        for which, head in every:
            near_out(which, head).wait_send()
            if head < HK - 1:
                own_back(which, head).wait_send()

    @pl.when(me == 2)
    def _():
        for which, head in every:
            near_on(which, head).wait_send()
            mix_on(which, head).wait_send()

        @pl.loop(0, heads)
        def _(which):
            q_back(which).wait_send()


def relay(queries, keys, values, segments):
    rows = queries.shape[1]
    heads = queries.shape[2] // HD
    width = 3 * rows
    stack = heads // HK * LANES
    anywhere = pl.BlockSpec(memory_space=pltpu.HBM)
    dma = pltpu.SemaphoreType.DMA
    both = dma((2, HK))
    return pl.pallas_call(
        relay_kernel,
        out_shape=pltpu.VMEM(queries.shape, BF16),
        in_specs=[anywhere] * 4,
        out_specs=pl.BlockSpec(memory_space=pltpu.VMEM),
        scratch_shapes=[
            pltpu.VMEM((rows, heads * HD), BF16),
            pltpu.VMEM((2, HK, width + rows, HD), BF16),
            pltpu.VMEM((3, 1, rows), jnp.int32),
            pltpu.VMEM((HK, width + rows, HD), BF16),
            pltpu.VMEM((HK, HD + 16, width + rows), BF16),
            pltpu.VMEM((HK, 2, stack, HD), BF16),
            pltpu.VMEM((HK, 2, 8, stack), F32),
            pltpu.VMEM((HK, 2, HD + 16, stack), F32),
            pltpu.VMEM((width + rows, HD), F32),
            pltpu.VMEM((width + rows, HD), F32),
            pltpu.VMEM((2, width, LANES), F32),
            pltpu.VMEM((heads, LANES, HD), BF16),
            pltpu.VMEM((heads, LANES, HD), BF16),
            pltpu.VMEM((heads // 2, 8, LANES), F32),
            pltpu.VMEM((heads // 2, 8, LANES), F32),
            pltpu.VMEM((LANES, HD), F32),
            pltpu.VMEM((LANES, HD), F32),
            pltpu.VMEM((3 * LANES, LANES), F32),
            pltpu.VMEM((8, LANES), F32),
            pltpu.VMEM((rows, heads * HD), BF16),
            pltpu.VMEM((HK, 2, stack, HD), BF16),
            pltpu.VMEM((2, width + rows, LANES), F32),
            pltpu.VMEM((rows, heads * HD), BF16),
            dma((2,)), dma, dma((2, HK, 2)), dma((3,)), dma((3,)), both, both, both, both,
            both, both, dma((heads,)), dma((heads,)), dma((heads // 2,)), dma((heads // 2,)),
            dma((heads,)), dma((heads,)), dma((HK,)), dma((HK,)), dma((HK,)), dma((HK,)),
        ],
        compiler_params=pltpu.CompilerParams(
            collective_id=0, has_side_effects=True, vmem_limit_bytes=60 * 1024 * 1024
        ),
        name="attend",
    )(queries, keys, values, segments)


def body(queries, keys, values, segments):
    count = lax.axis_size("ctx")
    hops = count // 2
    rows = queries.shape[1]
    width = (hops + 1) * rows
    span = hops * rows + LANES
    heads = queries.shape[2] // HD
    if count == 4 and rows == 2 * LANES and heads == 4 * HK:
        return relay(queries, keys, values, segments)
    anywhere = pl.BlockSpec(memory_space=pltpu.HBM)
    dma = pltpu.SemaphoreType.DMA
    return pl.pallas_call(
        functools.partial(kernel, count, hops),
        out_shape=pltpu.VMEM(queries.shape, BF16),
        in_specs=[anywhere] * 4,
        out_specs=pl.BlockSpec(memory_space=pltpu.VMEM),
        scratch_shapes=[
            pltpu.VMEM((rows, heads * HD), BF16),
            pltpu.VMEM((HK, width, HD), BF16),
            pltpu.VMEM((HK, width, HD), BF16),
            pltpu.VMEM((hops + 1, 1, rows), jnp.int32),
            pltpu.VMEM((width, HD), BF16),
            pltpu.VMEM((heads, rows, HD), BF16),
            pltpu.VMEM((heads, rows, span), BF16),
            pltpu.VMEM((heads, rows, LANES), F32),
            pltpu.VMEM((hops + 1, rows, HD), F32),
            pltpu.VMEM((hops + 1, rows, HD), F32),
            pltpu.VMEM((rows // LANES, LANES, span), F32),
            dma, dma, dma((2, HK)),
            dma((hops,)), dma((hops,)),
            dma((2, HK, hops)), dma((2, HK, hops)), dma((2, HK, hops)),
        ],
        compiler_params=pltpu.CompilerParams(
            collective_id=0, has_side_effects=True, vmem_limit_bytes=60 * 1024 * 1024
        ),
        name="attend",
    )(queries, keys, values, segments)


def solution(mesh):
    placed = (P("dp", "ctx", None), P("dp", "ctx", None), P("dp", "ctx", None), P("dp", "ctx"))
    return jax.shard_map(
        body, mesh=mesh, in_specs=placed, out_specs=P("dp", "ctx", None), check_vma=False
    )
```

```python
import functools
import math

import jax
import jax.numpy as jnp
from jax import lax
from jax.experimental import pallas as pl
from jax.experimental.pallas import tpu as pltpu
from jax.sharding import PartitionSpec as P

HK = 4
HD = 128
THETA = 500000.0
LANES = 128
MASKED = -1e30
F32 = jnp.float32
BF16 = jnp.bfloat16


def sin_cos(angle):
    turns = jnp.floor(angle * (2.0 / math.pi) + 0.5)
    rest = angle - turns * 1.5703125
    rest = rest - turns * 4.837512969970703125e-4
    rest = rest - turns * 7.54978995489188216e-8
    square = rest * rest
    sine = rest + rest * square * (
        -1.6666654611e-1 + square * (8.3321608736e-3 + square * -1.9515295891e-4)
    )
    cosine = (
        1.0
        - 0.5 * square
        + square * square * (4.166664568298827e-2 + square * (-1.388731625493765e-3 + square * 2.443315711809948e-5))
    )
    quarter = turns - 4.0 * jnp.floor(turns * 0.25)
    odd = (quarter == 1.0) | (quarter == 3.0)
    sin_out = jnp.where(odd, cosine, sine)
    cos_out = jnp.where(odd, sine, cosine)
    sin_out = jnp.where(quarter >= 2.0, -sin_out, sin_out)
    cos_out = jnp.where((quarter == 1.0) | (quarter == 2.0), -cos_out, cos_out)
    return sin_out, cos_out


def frequencies():
    index = lax.broadcasted_iota(jnp.int32, (1, HD), 1) % (HD // 2)
    result = jnp.ones((1, HD), F32)
    bit = 1
    while bit < HD // 2:
        factor = math.exp(-math.log(THETA) * 2.0 * bit / HD)
        result = result * jnp.where((index // bit) % 2 == 1, F32(factor), F32(1.0))
        bit *= 2
    return result


def turned(block, cosine, sine):
    block = block.astype(F32)
    return (block * cosine + pltpu.roll(block, HD // 2, 1) * sine).astype(BF16)


def kernel(
    count, hops, q_ref, k_ref, v_ref, seg_ref, out_ref,
    q_own, kwin, vwin, segwin, krot, qrot, weights, denoms, sines, cosines, bias,
    q_sem, seg_sem, own_sem, seg_send, seg_recv, send, recv, forward,
):
    me = lax.axis_index("ctx")
    rows = q_own.shape[0]
    span = bias.shape[2]
    group = qrot.shape[0] // HK
    windows = (kwin, vwin)

    def block(which, head, distance):
        return windows[which].at[head, pl.ds((hops - distance) * rows, rows)]

    own_copies = [
        [
            pltpu.make_async_copy(
                ref.at[0, :, pl.ds(head * HD, HD)], block(which, head, 0), own_sem.at[which, head]
            )
            for head in range(HK)
        ]
        for which, ref in enumerate((k_ref, v_ref))
    ]
    seg_copy = pltpu.make_async_copy(seg_ref, segwin.at[hops], seg_sem)
    q_copy = pltpu.make_async_copy(q_ref.at[0], q_own, q_sem)
    seg_copy.start()
    for which in range(2):
        for head in range(HK):
            own_copies[which][head].start()
    q_copy.start()

    barrier = pltpu.get_barrier_semaphore()
    for distance in range(1, hops + 1):
        @pl.when(me + distance < count)
        def _():
            pl.semaphore_signal(barrier, inc=1, device_id={"ctx": me + distance})

        @pl.when(me >= distance)
        def _():
            pl.semaphore_signal(barrier, inc=1, device_id={"ctx": me - distance})
    pl.semaphore_wait(barrier, jnp.minimum(me, hops) + jnp.minimum(count - 1 - me, hops))

    def seg_out(distance):
        return pltpu.make_async_remote_copy(
            src_ref=segwin.at[hops], dst_ref=segwin.at[hops - distance],
            send_sem=seg_send.at[distance - 1], recv_sem=seg_recv.at[distance - 1],
            device_id={"ctx": me + distance},
        )

    def block_out(which, head, distance):
        return pltpu.make_async_remote_copy(
            src_ref=block(which, head, 0), dst_ref=block(which, head, distance),
            send_sem=send.at[which, head, distance - 1], recv_sem=recv.at[which, head, distance - 1],
            device_id={"ctx": me + distance},
        )

    def block_on(which, head, distance):
        return pltpu.make_async_remote_copy(
            src_ref=block(which, head, distance), dst_ref=block(which, head, distance + 1),
            send_sem=forward.at[which, head, distance - 1], recv_sem=recv.at[which, head, distance],
            device_id={"ctx": me + 1},
        )

    def goes_out(distance):
        direct = me + distance < count
        if distance > 1:
            direct = direct & ((me + distance) % 2 == 0)
        return direct

    def goes_on(distance):
        return (me % 2 == 0) & (me >= distance) & (me + 1 < count)

    seg_copy.wait()
    for distance in range(1, hops + 1):
        @pl.when(me + distance < count)
        def _():
            seg_out(distance).start()
    for which in range(2):
        for head in range(HK):
            own_copies[which][head].wait()

            @pl.when(goes_out(1))
            def _():
                block_out(which, head, 1).start()
    for distance in range(2, hops + 1):
        @pl.when(goes_out(distance))
        def _():
            for which in range(2):
                for head in range(HK):
                    if distance == 2:
                        block_out(which, head, 1).wait_send()
                    block_out(which, head, distance).start()

    for distance in range(1, hops + 1):
        @pl.when(me < distance)
        def _():
            empty = jnp.zeros((HK, rows, HD), BF16)
            kwin[:, pl.ds((hops - distance) * rows, rows)] = empty
            vwin[:, pl.ds((hops - distance) * rows, rows)] = empty
            segwin[hops - distance] = jnp.full((1, rows), -1, jnp.int32)

    for distance in range(1, hops + 1):
        @pl.when(me >= distance)
        def _():
            seg_out(distance).wait_recv()

    freq = frequencies()
    lane = lax.broadcasted_iota(jnp.int32, (rows, LANES), 1)
    row = lax.broadcasted_iota(jnp.int32, (rows, LANES), 0)
    sign = jnp.where(lane < HD // 2, F32(-1.0), F32(1.0))
    ones = jnp.ones((LANES, LANES), BF16)
    pieces = []
    for index in range(hops + 1):
        seg_row = segwin[index].astype(F32)
        pieces += [seg_row[:, at:at + LANES] for at in range(0, rows, LANES)]
    for index in range(hops + 1):
        column = jnp.broadcast_to(segwin[index].astype(F32), (LANES, rows)).T
        smaller = jnp.zeros((rows, LANES), F32)
        for piece in pieces:
            smaller = smaller + jnp.where(piece < column, F32(1.0), F32(0.0))
        start = jnp.dot(smaller.astype(BF16), ones, preferred_element_type=F32)
        position = (row + index * rows).astype(F32) - start
        sine, cosine = sin_cos(position * freq)
        sines[index] = sine * sign
        cosines[index] = cosine
        if index == hops:
            last = (row + hops * rows).astype(F32)
            for tile in range(rows // LANES):
                mine = slice(tile * LANES, (tile + 1) * LANES)
                for at in range(0, span, LANES):
                    spot = (lane[mine] + (at + tile * LANES)).astype(F32)
                    bias[tile, :, at:at + LANES] = jnp.where(
                        (spot >= start[mine]) & (spot <= last[mine]), F32(0.0), F32(MASKED)
                    )

    q_copy.wait()

    @pl.loop(0, qrot.shape[0])
    def _(head):
        at = pl.ds(pl.multiple_of(head * HD, HD), HD)
        qrot[head] = turned(q_own[:, at], cosines[hops], sines[hops])

    scale = F32(math.log2(math.e) / math.sqrt(HD))

    def arrive(head, distance, which):
        @pl.when(me >= distance)
        def _():
            block_out(which, head, distance).wait_recv()
        if distance < hops:
            @pl.when(goes_on(distance))
            def _():
                block_on(which, head, distance).start()

    @pl.loop(0, HK)
    def _(head):
        for distance in range(1, hops + 1):
            arrive(head, distance, 0)
        for index in range(hops + 1):
            at = pl.ds(index * rows, rows)
            krot[at] = turned(kwin[head, at], cosines[index], sines[index])

        for part in range(group):
            for tile in range(rows // LANES):
                mine = slice(tile * LANES, (tile + 1) * LANES)
                seen = pl.ds(tile * LANES, span)
                scores = lax.dot_general(
                    qrot[head * group + part, mine], krot[seen], (((1,), (1,)), ((), ())),
                    preferred_element_type=F32,
                ) + bias[tile]
                top = jnp.max(scores, axis=1, keepdims=True)
                weight = jnp.exp2((scores - top) * scale)
                denoms[head * group + part, mine] = jnp.broadcast_to(
                    jnp.sum(weight, axis=1, keepdims=True), (LANES, LANES)
                )
                weights[head * group + part, mine] = weight.astype(BF16)

    for distance in range(1, hops):
        arrive(0, distance, 1)

    @pl.loop(0, HK)
    def _(head):
        @pl.when(head + 1 < HK)
        def _():
            for distance in range(1, hops):
                arrive(head + 1, distance, 1)

        arrive(head, hops, 1)

        for part in range(group):
            for tile in range(rows // LANES):
                mine = slice(tile * LANES, (tile + 1) * LANES)
                seen = pl.ds(tile * LANES, span)
                total = jnp.dot(weights[head * group + part, mine], vwin[head, seen], preferred_element_type=F32)
                at = pl.ds(pl.multiple_of((head * group + part) * HD, HD), HD)
                out_ref[0, mine, at] = (total / denoms[head * group + part, mine]).astype(BF16)

    for distance in range(1, hops + 1):
        @pl.when(me + distance < count)
        def _():
            seg_out(distance).wait_send()
        unsent = goes_out(distance)
        if distance == 1 and hops > 1:
            unsent = unsent & jnp.logical_not(goes_out(2))
        for which in range(2):
            for head in range(HK):
                @pl.when(unsent)
                def _():
                    block_out(which, head, distance).wait_send()
                if distance < hops:
                    @pl.when(goes_on(distance))
                    def _():
                        block_on(which, head, distance).wait_send()


def relay_kernel(
    q_ref, k_ref, v_ref, seg_ref, out_ref,
    q_own, win, segwin, krot, vturn, qrot, tops, totals, sines, cosines, bias,
    q_in, mix, mixed, lse_out, lse_in, q_sine, q_cosine, q_bias, mark, q_next, next_rot, next_bias, next_out,
    q_sem, seg_sem, own_sem, seg_send, seg_recv, back_send, back_recv, own_send, own_recv,
    near_send, near_recv, mix_send, mix_recv, lse_send, lse_recv, q_send, q_recv,
    help_send, help_recv, give_send, give_recv,
):
    me = lax.axis_index("ctx")
    count = lax.axis_size("ctx")
    rows = q_own.shape[0]
    heads = q_own.shape[1] // HD
    group = heads // HK
    scale = F32(math.log2(math.e) / math.sqrt(HD))

    def blocks(first, last):
        if isinstance(first, int):
            return pl.ds(first * LANES, (last - first) * LANES)
        return pl.ds(pl.multiple_of(first * LANES, LANES), LANES)

    def columns(head):
        return pl.ds(head * HD if isinstance(head, int) else pl.multiple_of(head * HD, HD), HD)

    def duo(pair):
        at = pair * 2 * HD
        return pl.ds(at if isinstance(pair, int) else pl.multiple_of(at, 2 * HD), 2 * HD)

    sources = (k_ref, v_ref)
    own, before, after = blocks(4, 6), blocks(2, 4), blocks(6, 8)
    own_copies = [
        pltpu.make_async_copy(sources[which].at[0], win.at[which, own], own_sem.at[which]) for which in range(2)
    ]
    seg_copy = pltpu.make_async_copy(seg_ref, segwin.at[2], seg_sem)
    q_copy = pltpu.make_async_copy(q_ref.at[0], q_own, q_sem)
    tail = pl.ds((HK - 1) * group * HD, group * HD)
    keep_copy = pltpu.make_async_copy(q_ref.at[0, :, tail], q_own.at[:, tail], q_sem)
    seg_copy.start()

    barrier = pltpu.get_barrier_semaphore()

    def greet(step, here):
        @pl.when(here)
        def _():
            pl.semaphore_signal(barrier, inc=1, device_id={"ctx": me + step})

    greet(1, me + 1 < count)
    greet(-1, me >= 1)
    greet(2, me + 2 < count)
    greet(-2, me >= 2)

    pl.semaphore_wait(barrier, jnp.minimum(me, 2) + jnp.minimum(count - 1 - me, 2))

    def remote(source, target, sent, received, there):
        return pltpu.make_async_remote_copy(
            src_ref=source, dst_ref=target, send_sem=sent, recv_sem=received, device_id={"ctx": there}
        )

    def seg_out(distance):
        return remote(
            segwin.at[2], segwin.at[2 - distance], seg_send.at[distance - 1], seg_recv.at[distance - 1], me + distance
        )

    def seg_back():
        return remote(segwin.at[2], segwin.at[1], seg_send.at[2], seg_recv.at[2], me - 1)

    def own_out(which):
        return remote(sources[which].at[0], win.at[which, before], own_send, own_recv.at[which], me + 1)

    def own_back(which):
        return remote(sources[which].at[0], win.at[which, after], back_send, back_recv.at[which], me - 1)

    helped = pl.ds(0, (HK - 1) * group * HD)

    def help_out():
        return remote(q_ref.at[0, :, helped], q_next.at[:, helped], help_send, help_recv, me - 1)

    def give_out(head):
        width = group * HD
        at = pl.ds(head * width if isinstance(head, int) else pl.multiple_of(head * width, width), width)
        return remote(next_out.at[:, at], out_ref.at[0, :, at], give_send, give_recv.at[head], me + 1)

    quarters = [(which, part) for part in range(2) for which in range(2)]

    def near_out(which, part):
        return remote(
            sources[which].at[0, blocks(1, 2), duo(part)], win.at[which, blocks(3, 4), duo(part)],
            near_send, near_recv.at[which, part], me + 1,
        )

    def near_on(which, part):
        return remote(
            win.at[which, blocks(3, 4), duo(part)], win.at[which, blocks(1, 2), duo(part)],
            near_send, near_recv.at[which, part], me + 1,
        )

    def mix_out(pair):
        return remote(mix.at[pair], mixed.at[pair], mix_send, mix_recv.at[pair], me + 1)

    def mix_on(head):
        return remote(mixed.at[head], mixed.at[head], mix_send, mix_recv.at[head], me + 1)

    few = pl.ds(0, group)

    def lse_copy(head):
        return remote(lse_out.at[head, few], lse_in.at[head, few], lse_send, lse_recv.at[head], me + 1)

    def q_back(pair):
        return remote(q_ref.at[0, blocks(0, 1), duo(pair)], q_in.at[pair], q_send, q_recv.at[pair], me - 1)

    def all_sent(ref, sent, received):
        remote(ref, ref, sent, received, me + 1).wait_send()

    freq = frequencies()
    lane = lax.broadcasted_iota(jnp.int32, (LANES, LANES), 1)
    row = lax.broadcasted_iota(jnp.int32, (LANES, LANES), 0)
    sign = jnp.where(lane < HD // 2, F32(-1.0), F32(1.0))
    ones = jnp.ones((LANES, LANES), BF16)

    def start_of(index, pieces):
        column = jnp.broadcast_to(segwin[index].astype(F32), (LANES, rows)).T
        smaller = jnp.zeros((rows, LANES), F32)
        for piece in pieces:
            smaller = smaller + jnp.where(piece < column, F32(1.0), F32(0.0))
        return jnp.dot(smaller.astype(BF16), ones, preferred_element_type=F32)

    def tables(start, block):
        sine, cosine = sin_cos(((row + block * LANES).astype(F32) - start) * freq)
        at = blocks(block, block + 1)
        sines[at] = sine * sign
        cosines[at] = cosine

    def masks(where, start, tile, low, own):
        first = start.T
        last = (lane + (own + tile) * LANES).astype(F32)
        for block in range(low, own + 1 + tile):
            key = (row + block * LANES).astype(F32)
            live = key >= first
            if block == own + tile:
                live = live & (key <= last)
            where[tile, blocks(block, block + 1)] = jnp.where(live, F32(0.0), F32(MASKED))

    def turn(head, block, keys, values):
        at = blocks(block, block + 1)
        krot[head, at] = turned(keys, cosines[at], sines[at])
        vturn[head, 0:HD, at] = values.T

    def turn_key(head, block):
        at = blocks(block, block + 1)
        turn(head, block, win[0, at, columns(head)], win[1, at, columns(head)])

    def turn_queries(head, source, target, own):
        for tile in range(2):
            place = blocks(own + tile, own + 1 + tile)
            cosine, sine = cosines[place], sines[place]
            for member in range(group):
                target[head, tile, blocks(member, member + 1)] = turned(
                    source[blocks(tile, tile + 1), columns(head * group + member)], cosine, sine
                )

    def raw_scores(keys, one):
        return lax.dot_general(keys, one, (((1,), (1,)), ((), ())), preferred_element_type=F32)

    def spread(part):
        return jnp.concatenate([part] * group, axis=1)

    def scores_of(head, tile, first, last):
        at = blocks(first, last)
        return raw_scores(krot[head, at], qrot[head, tile]) + spread(bias[tile, at])

    def summed(head, weight, at):
        return jnp.dot(vturn[head, :, at], weight.astype(BF16), preferred_element_type=F32)

    def keep(head, tile, top, both):
        tops[head, tile] = jnp.broadcast_to(top, tops.shape[2:])
        totals[head, tile] = both

    def put(head, tile, total, under, target=None):
        value = (total * (1.0 / under)).astype(BF16)
        for member in range(group):
            done = value[:, member * LANES:(member + 1) * LANES].T
            if target is None:
                out_ref[0, blocks(tile, tile + 1), columns(head * group + member)] = done
            else:
                target[blocks(tile, tile + 1), columns(head * group + member)] = done

    def fresh(head, first, last=5, ones=qrot, mask=bias):
        found = []
        for tile in range(2):
            at = blocks(first, last + tile)
            found.append(raw_scores(krot[head, at], ones[head, tile]) + spread(mask[tile, at]))
        result = []
        for tile in range(2):
            top = jnp.max(found[tile], axis=0, keepdims=True)
            weight = jnp.exp2((found[tile] - top) * scale)
            result.append((top, summed(head, weight, blocks(first, last + tile))))
        return result

    def more(head, tile, scores, first, last, extra=None):
        old = tops[head, tile, 0:1]
        top = jnp.maximum(old, jnp.max(scores, axis=0, keepdims=True))
        if extra is not None:
            top = jnp.maximum(top, extra)
        ratio = jnp.exp2((old - top) * scale)
        weight = jnp.exp2((scores - top) * scale)
        return top, totals[head, tile] * ratio + summed(head, weight, blocks(first, last))

    seg_copy.wait()
    for distance in (1, 2):
        @pl.when(me + distance < count)
        def _():
            seg_out(distance).start()

    @pl.when(me == 1)
    def _():
        seg_back().start()

    @pl.when(me == 2)
    def _():
        for pair in range(heads // 2):
            q_back(pair).start()

    @pl.when(me == 1)
    def _():
        for which, part in quarters:
            near_out(which, part).start()
        for which in range(2):
            own_back(which).start()
        help_out().start()

    @pl.when(me % 2 == 0)
    def _():
        for which in range(2):
            own_out(which).start()

    for which in range(2):
        own_copies[which].start()

    @pl.when(me == 1)
    def _():
        keep_copy.start()

    @pl.when(me != 1)
    def _():
        q_copy.start()

    @pl.when(me <= 1)
    def _():
        segwin[0] = jnp.full((1, rows), -1, jnp.int32)

    @pl.when(me == 0)
    def _():
        seg_back().wait_recv()

    for distance in (1, 2):
        @pl.when(me >= distance)
        def _():
            seg_out(distance).wait_recv()

    for which in range(2):
        own_copies[which].wait()

    pieces = []
    for index in range(3):
        seg_row = segwin[index].astype(F32)
        pieces += [seg_row[:, at:at + LANES] for at in range(0, rows, LANES)]
    shift = jnp.where(me == 0, rows, 0).astype(F32)
    begin = start_of(2, pieces) + shift
    start = start_of(1, pieces) + shift
    vturn[:, HD:] = jnp.ones((HK, vturn.shape[1] - HD, vturn.shape[2]), BF16)
    tables(begin[:LANES], 4)
    for tile in range(2):
        tables(start[tile * LANES:(tile + 1) * LANES], jnp.where(me == 0, 6, 2) + tile)

    @pl.when(me == 1)
    def _():
        late = begin[rows - 1:rows]
        sine, cosine = sin_cos(((row + 6 * LANES).astype(F32) - late) * freq)
        q_sine[...] = sine * sign
        q_cosine[...] = cosine
        for block in range(3):
            key = (row + (2 + block) * LANES).astype(F32)
            q_bias[blocks(block, block + 1)] = jnp.where(key >= late, F32(0.0), F32(MASKED))
        given = late < F32(3 * LANES)
        seen = blocks(2, 5)
        for head in range(HK):
            turn_key(head, 4)
        for which in range(2):
            own_out(which).wait_recv()

        @pl.loop(0, HK)
        def _(head):
            turn_key(head, 2)
            turn_key(head, 3)
            for part in range(group // 2):
                pair = 2 * head + part
                q_back(pair).wait_recv()
                one = jnp.concatenate(
                    [
                        turned(q_in[pair, :, member * HD:(member + 1) * HD], q_cosine[...], q_sine[...])
                        for member in range(2)
                    ],
                    axis=0,
                )
                scores = raw_scores(krot[head, seen], one) + jnp.concatenate([q_bias[...]] * 2, axis=1)
                top = jnp.max(scores, axis=0, keepdims=True)
                both = summed(head, jnp.exp2((scores - top) * scale), seen)
                under = both[HD:HD + 1]
                total = both[:HD] * (1.0 / under)
                place = blocks(4 - pair // HK, None)
                for member in range(2):
                    mix[pair, member] = jnp.where(
                        given, total[:, member * LANES:(member + 1) * LANES],
                        win[member, place, columns(pair % HK)].astype(F32),
                    ).astype(BF16)
                lse = top + jnp.log(under) * F32(math.sqrt(HD))
                for member in range(2):
                    at = 2 * part + member
                    lse_out[head, at:at + 1] = lse[:, member * LANES:(member + 1) * LANES]
                mix_out(pair).start()
            lse_copy(head).start()

    tables(begin[LANES:], 5)
    mark[...] = begin[:LANES].T[:8]
    first = jnp.where((begin < F32(LANES)) & (me == 2), F32(3 * LANES), begin)
    for tile in range(2):
        masks(bias, first[tile * LANES:(tile + 1) * LANES], tile, 0, 4)

    @pl.when(me == 1)
    def _():
        keep_copy.wait()
        head = HK - 1
        turn_queries(head, q_own, qrot, 4)
        turn_key(head, 5)
        for tile, (top, both) in enumerate(fresh(head, 2)):
            put(head, tile, both[:HD], both[HD:HD + 1])

    @pl.when(me == 0)
    def _():
        for tile in range(2):
            masks(next_bias, start[tile * LANES:(tile + 1) * LANES], tile, 4, 6)
        q_copy.wait()

        @pl.loop(0, HK)
        def _(head):
            turn_queries(head, q_own, qrot, 4)
            for block in (4, 5):
                turn_key(head, block)
            for tile, (top, both) in enumerate(fresh(head, 4)):
                put(head, tile, both[:HD], both[HD:HD + 1])

        for which in range(2):
            own_back(which).wait_recv()
        help_out().wait_recv()

        @pl.loop(0, HK - 1)
        def _(head):
            turn_queries(head, q_next, next_rot, 6)
            for block in (6, 7):
                turn_key(head, block)
            for tile, (top, both) in enumerate(fresh(head, 4, 7, next_rot, next_bias)):
                put(head, tile, both[:HD], both[HD:HD + 1], next_out)
            give_out(head).start()

    @pl.when(me >= 2)
    def _():
        start = start_of(0, pieces)
        for tile in range(2):
            tables(start[tile * LANES:(tile + 1) * LANES], tile)

        q_copy.wait()

        @pl.loop(0, HK)
        def _(head):
            turn_queries(head, q_own, qrot, 4)
            for block in (4, 5):
                turn_key(head, block)

    @pl.when(me == 2)
    def _():
        for which, part in quarters:
            near_out(which, part).wait_recv()
            near_on(which, part).start()

        @pl.loop(0, HK)
        def _(head):
            turn_key(head, 3)
            for tile, (top, both) in enumerate(fresh(head, 3)):
                keep(head, tile, top, both)

        @pl.loop(0, HK)
        def _(head):
            mix_out(head).wait_recv()
            mix_on(head).start()
            turn(head, 2, mixed[head, 0], mixed[head, 1])
            found = [scores_of(head, tile, 2, 3) for tile in range(2)]
            for tile in range(2):
                keep(head, tile, *more(head, tile, found[tile], 2, 3))

        @pl.loop(0, HK)
        def _(head):
            mix_out(HK + head).wait_recv()
            lse_copy(head).wait_recv()
            turn(head, 1, mixed[HK + head, 0], mixed[HK + head, 1])
            found = [scores_of(head, tile, 1, 2) for tile in range(2)]
            crossing = spread(mark[0:1] < F32(LANES))
            lse = jnp.concatenate([lse_in[head, member:member + 1] for member in range(group)], axis=1)
            lse = jnp.where(crossing, lse, F32(MASKED))
            top, both = more(head, 0, found[0], 1, 2, lse)
            share = jnp.exp2((lse - top) * scale)
            given = jnp.concatenate(
                [mixed[2 * head + member // 2, member % 2] for member in range(group)], axis=1
            )
            put(head, 0, both[:HD] + given.astype(F32) * share, both[HD:HD + 1] + share)
            top, both = more(head, 1, found[1], 1, 2)
            put(head, 1, both[:HD], both[HD:HD + 1])

    @pl.when(me == 3)
    def _():
        for which in range(2):
            own_out(which).wait_recv()

        @pl.loop(0, HK)
        def _(head):
            for block in (2, 3):
                turn_key(head, block)
            for tile, (top, both) in enumerate(fresh(head, 2)):
                keep(head, tile, top, both)

        for which, part in quarters:
            near_on(which, part).wait_recv()

        @pl.loop(0, HK)
        def _(head):
            mix_on(head).wait_recv()
            turn(head, 0, mixed[head, 0], mixed[head, 1])
            turn_key(head, 1)
            found = [scores_of(head, tile, tile, 2) for tile in range(2)]
            for tile in range(2):
                top, both = more(head, tile, found[tile], tile, 2)
                put(head, tile, both[:HD], both[HD:HD + 1])

    for distance in (1, 2):
        @pl.when(me + distance < count)
        def _():
            seg_out(distance).wait_send()

    @pl.when(me % 2 == 0)
    def _():
        all_sent(win.at[:, own], own_send, own_recv.at[0])

    @pl.when(me == 0)
    def _():
        all_sent(next_out.at[:, helped], give_send, give_recv.at[0])

    @pl.when(me == 1)
    def _():
        seg_back().wait_send()
        all_sent(win.at[:, blocks(3, 4)], near_send, near_recv.at[0, 0])
        all_sent(win.at[:, own], back_send, back_recv.at[0])
        help_out().wait_send()
        all_sent(mix, mix_send, mix_recv.at[0])
        all_sent(lse_out.at[:, few], lse_send, lse_recv.at[0])
        for head in range(HK - 1):
            give_out(head).wait_recv()

    @pl.when(me == 2)
    def _():
        all_sent(win.at[:, blocks(3, 4)], near_send, near_recv.at[0, 0])
        all_sent(mixed.at[pl.ds(0, HK)], mix_send, mix_recv.at[0])
        all_sent(q_own.at[blocks(0, 1)], q_send, q_recv.at[0])


def relay(queries, keys, values, segments):
    rows = queries.shape[1]
    heads = queries.shape[2] // HD
    width = 3 * rows
    stack = heads // HK * LANES
    anywhere = pl.BlockSpec(memory_space=pltpu.HBM)
    dma = pltpu.SemaphoreType.DMA
    return pl.pallas_call(
        relay_kernel,
        out_shape=pltpu.VMEM(queries.shape, BF16),
        in_specs=[anywhere] * 4,
        out_specs=pl.BlockSpec(memory_space=pltpu.VMEM),
        scratch_shapes=[
            pltpu.VMEM((rows, heads * HD), BF16),
            pltpu.VMEM((2, width + rows, HK * HD), BF16),
            pltpu.VMEM((3, 1, rows), jnp.int32),
            pltpu.VMEM((HK, width + rows, HD), BF16),
            pltpu.VMEM((HK, HD + 16, width + rows), BF16),
            pltpu.VMEM((HK, 2, stack, HD), BF16),
            pltpu.VMEM((HK, 2, 8, stack), F32),
            pltpu.VMEM((HK, 2, HD + 16, stack), F32),
            pltpu.VMEM((width + rows, HD), F32),
            pltpu.VMEM((width + rows, HD), F32),
            pltpu.VMEM((2, width, LANES), F32),
            pltpu.VMEM((heads // 2, LANES, 2 * HD), BF16),
            pltpu.VMEM((heads // 2, 2, LANES, HD), BF16),
            pltpu.VMEM((heads // 2, 2, LANES, HD), BF16),
            pltpu.VMEM((HK, 8, LANES), F32),
            pltpu.VMEM((HK, 8, LANES), F32),
            pltpu.VMEM((LANES, HD), F32),
            pltpu.VMEM((LANES, HD), F32),
            pltpu.VMEM((3 * LANES, LANES), F32),
            pltpu.VMEM((8, LANES), F32),
            pltpu.VMEM((rows, heads * HD), BF16),
            pltpu.VMEM((HK, 2, stack, HD), BF16),
            pltpu.VMEM((2, width + rows, LANES), F32),
            pltpu.VMEM((rows, heads * HD), BF16),
            dma, dma, dma((2,)), dma((3,)), dma((3,)), dma, dma((2,)), dma, dma((2,)),
            dma, dma((2, 2)), dma, dma((heads // 2,)), dma, dma((HK,)), dma, dma((heads // 2,)),
            dma, dma, dma, dma((HK - 1,)),
        ],
        compiler_params=pltpu.CompilerParams(
            collective_id=0, has_side_effects=True, vmem_limit_bytes=60 * 1024 * 1024
        ),
        name="attend",
    )(queries, keys, values, segments)


def body(queries, keys, values, segments):
    count = lax.axis_size("ctx")
    hops = count // 2
    rows = queries.shape[1]
    width = (hops + 1) * rows
    span = hops * rows + LANES
    heads = queries.shape[2] // HD
    if count == 4 and rows == 2 * LANES and heads == 4 * HK:
        return relay(queries, keys, values, segments)
    anywhere = pl.BlockSpec(memory_space=pltpu.HBM)
    dma = pltpu.SemaphoreType.DMA
    return pl.pallas_call(
        functools.partial(kernel, count, hops),
        out_shape=pltpu.VMEM(queries.shape, BF16),
        in_specs=[anywhere] * 4,
        out_specs=pl.BlockSpec(memory_space=pltpu.VMEM),
        scratch_shapes=[
            pltpu.VMEM((rows, heads * HD), BF16),
            pltpu.VMEM((HK, width, HD), BF16),
            pltpu.VMEM((HK, width, HD), BF16),
            pltpu.VMEM((hops + 1, 1, rows), jnp.int32),
            pltpu.VMEM((width, HD), BF16),
            pltpu.VMEM((heads, rows, HD), BF16),
            pltpu.VMEM((heads, rows, span), BF16),
            pltpu.VMEM((heads, rows, LANES), F32),
            pltpu.VMEM((hops + 1, rows, HD), F32),
            pltpu.VMEM((hops + 1, rows, HD), F32),
            pltpu.VMEM((rows // LANES, LANES, span), F32),
            dma, dma, dma((2, HK)),
            dma((hops,)), dma((hops,)),
            dma((2, HK, hops)), dma((2, HK, hops)), dma((2, HK, hops)),
        ],
        compiler_params=pltpu.CompilerParams(
            collective_id=0, has_side_effects=True, vmem_limit_bytes=60 * 1024 * 1024
        ),
        name="attend",
    )(queries, keys, values, segments)


def solution(mesh):
    placed = (P("dp", "ctx", None), P("dp", "ctx", None), P("dp", "ctx", None), P("dp", "ctx"))
    return jax.shard_map(
        body, mesh=mesh, in_specs=placed, out_specs=P("dp", "ctx", None), check_vma=False
    )
```

```python
import functools
import math

import jax
import jax.numpy as jnp
from jax import lax
from jax.experimental import pallas as pl
from jax.experimental.pallas import tpu as pltpu
from jax.sharding import PartitionSpec as P

HK = 4
HD = 128
THETA = 500000.0
LANES = 128
MASKED = -1e30
F32 = jnp.float32
BF16 = jnp.bfloat16


def sin_cos(angle):
    turns = jnp.floor(angle * (2.0 / math.pi) + 0.5)
    rest = angle - turns * 1.5703125
    rest = rest - turns * 4.837512969970703125e-4
    rest = rest - turns * 7.54978995489188216e-8
    square = rest * rest
    sine = rest + rest * square * (
        -1.6666654611e-1 + square * (8.3321608736e-3 + square * -1.9515295891e-4)
    )
    cosine = (
        1.0
        - 0.5 * square
        + square * square * (4.166664568298827e-2 + square * (-1.388731625493765e-3 + square * 2.443315711809948e-5))
    )
    quarter = turns - 4.0 * jnp.floor(turns * 0.25)
    odd = (quarter == 1.0) | (quarter == 3.0)
    sin_out = jnp.where(odd, cosine, sine)
    cos_out = jnp.where(odd, sine, cosine)
    sin_out = jnp.where(quarter >= 2.0, -sin_out, sin_out)
    cos_out = jnp.where((quarter == 1.0) | (quarter == 2.0), -cos_out, cos_out)
    return sin_out, cos_out


def frequencies():
    index = lax.broadcasted_iota(jnp.int32, (1, HD), 1) % (HD // 2)
    result = jnp.ones((1, HD), F32)
    bit = 1
    while bit < HD // 2:
        factor = math.exp(-math.log(THETA) * 2.0 * bit / HD)
        result = result * jnp.where((index // bit) % 2 == 1, F32(factor), F32(1.0))
        bit *= 2
    return result


def turned(block, cosine, sine):
    block = block.astype(F32)
    return (block * cosine + pltpu.roll(block, HD // 2, 1) * sine).astype(BF16)


def kernel(
    count, hops, q_ref, k_ref, v_ref, seg_ref, out_ref,
    q_own, kwin, vwin, segwin, krot, qrot, weights, denoms, sines, cosines, bias,
    q_sem, seg_sem, own_sem, seg_send, seg_recv, send, recv, forward,
):
    me = lax.axis_index("ctx")
    rows = q_own.shape[0]
    span = bias.shape[2]
    group = qrot.shape[0] // HK
    windows = (kwin, vwin)

    def block(which, head, distance):
        return windows[which].at[head, pl.ds((hops - distance) * rows, rows)]

    own_copies = [
        [
            pltpu.make_async_copy(
                ref.at[0, :, pl.ds(head * HD, HD)], block(which, head, 0), own_sem.at[which, head]
            )
            for head in range(HK)
        ]
        for which, ref in enumerate((k_ref, v_ref))
    ]
    seg_copy = pltpu.make_async_copy(seg_ref, segwin.at[hops], seg_sem)
    q_copy = pltpu.make_async_copy(q_ref.at[0], q_own, q_sem)
    seg_copy.start()
    for which in range(2):
        for head in range(HK):
            own_copies[which][head].start()
    q_copy.start()

    barrier = pltpu.get_barrier_semaphore()
    for distance in range(1, hops + 1):
        @pl.when(me + distance < count)
        def _():
            pl.semaphore_signal(barrier, inc=1, device_id={"ctx": me + distance})

        @pl.when(me >= distance)
        def _():
            pl.semaphore_signal(barrier, inc=1, device_id={"ctx": me - distance})
    pl.semaphore_wait(barrier, jnp.minimum(me, hops) + jnp.minimum(count - 1 - me, hops))

    def seg_out(distance):
        return pltpu.make_async_remote_copy(
            src_ref=segwin.at[hops], dst_ref=segwin.at[hops - distance],
            send_sem=seg_send.at[distance - 1], recv_sem=seg_recv.at[distance - 1],
            device_id={"ctx": me + distance},
        )

    def block_out(which, head, distance):
        return pltpu.make_async_remote_copy(
            src_ref=block(which, head, 0), dst_ref=block(which, head, distance),
            send_sem=send.at[which, head, distance - 1], recv_sem=recv.at[which, head, distance - 1],
            device_id={"ctx": me + distance},
        )

    def block_on(which, head, distance):
        return pltpu.make_async_remote_copy(
            src_ref=block(which, head, distance), dst_ref=block(which, head, distance + 1),
            send_sem=forward.at[which, head, distance - 1], recv_sem=recv.at[which, head, distance],
            device_id={"ctx": me + 1},
        )

    def goes_out(distance):
        direct = me + distance < count
        if distance > 1:
            direct = direct & ((me + distance) % 2 == 0)
        return direct

    def goes_on(distance):
        return (me % 2 == 0) & (me >= distance) & (me + 1 < count)

    seg_copy.wait()
    for distance in range(1, hops + 1):
        @pl.when(me + distance < count)
        def _():
            seg_out(distance).start()
    for which in range(2):
        for head in range(HK):
            own_copies[which][head].wait()

            @pl.when(goes_out(1))
            def _():
                block_out(which, head, 1).start()
    for distance in range(2, hops + 1):
        @pl.when(goes_out(distance))
        def _():
            for which in range(2):
                for head in range(HK):
                    if distance == 2:
                        block_out(which, head, 1).wait_send()
                    block_out(which, head, distance).start()

    for distance in range(1, hops + 1):
        @pl.when(me < distance)
        def _():
            empty = jnp.zeros((HK, rows, HD), BF16)
            kwin[:, pl.ds((hops - distance) * rows, rows)] = empty
            vwin[:, pl.ds((hops - distance) * rows, rows)] = empty
            segwin[hops - distance] = jnp.full((1, rows), -1, jnp.int32)

    for distance in range(1, hops + 1):
        @pl.when(me >= distance)
        def _():
            seg_out(distance).wait_recv()

    freq = frequencies()
    lane = lax.broadcasted_iota(jnp.int32, (rows, LANES), 1)
    row = lax.broadcasted_iota(jnp.int32, (rows, LANES), 0)
    sign = jnp.where(lane < HD // 2, F32(-1.0), F32(1.0))
    ones = jnp.ones((LANES, LANES), BF16)
    pieces = []
    for index in range(hops + 1):
        seg_row = segwin[index].astype(F32)
        pieces += [seg_row[:, at:at + LANES] for at in range(0, rows, LANES)]
    for index in range(hops + 1):
        column = jnp.broadcast_to(segwin[index].astype(F32), (LANES, rows)).T
        smaller = jnp.zeros((rows, LANES), F32)
        for piece in pieces:
            smaller = smaller + jnp.where(piece < column, F32(1.0), F32(0.0))
        start = jnp.dot(smaller.astype(BF16), ones, preferred_element_type=F32)
        position = (row + index * rows).astype(F32) - start
        sine, cosine = sin_cos(position * freq)
        sines[index] = sine * sign
        cosines[index] = cosine
        if index == hops:
            last = (row + hops * rows).astype(F32)
            for tile in range(rows // LANES):
                mine = slice(tile * LANES, (tile + 1) * LANES)
                for at in range(0, span, LANES):
                    spot = (lane[mine] + (at + tile * LANES)).astype(F32)
                    bias[tile, :, at:at + LANES] = jnp.where(
                        (spot >= start[mine]) & (spot <= last[mine]), F32(0.0), F32(MASKED)
                    )

    q_copy.wait()

    @pl.loop(0, qrot.shape[0])
    def _(head):
        at = pl.ds(pl.multiple_of(head * HD, HD), HD)
        qrot[head] = turned(q_own[:, at], cosines[hops], sines[hops])

    scale = F32(math.log2(math.e) / math.sqrt(HD))

    def arrive(head, distance, which):
        @pl.when(me >= distance)
        def _():
            block_out(which, head, distance).wait_recv()
        if distance < hops:
            @pl.when(goes_on(distance))
            def _():
                block_on(which, head, distance).start()

    @pl.loop(0, HK)
    def _(head):
        for distance in range(1, hops + 1):
            arrive(head, distance, 0)
        for index in range(hops + 1):
            at = pl.ds(index * rows, rows)
            krot[at] = turned(kwin[head, at], cosines[index], sines[index])

        for part in range(group):
            for tile in range(rows // LANES):
                mine = slice(tile * LANES, (tile + 1) * LANES)
                seen = pl.ds(tile * LANES, span)
                scores = lax.dot_general(
                    qrot[head * group + part, mine], krot[seen], (((1,), (1,)), ((), ())),
                    preferred_element_type=F32,
                ) + bias[tile]
                top = jnp.max(scores, axis=1, keepdims=True)
                weight = jnp.exp2((scores - top) * scale)
                denoms[head * group + part, mine] = jnp.broadcast_to(
                    jnp.sum(weight, axis=1, keepdims=True), (LANES, LANES)
                )
                weights[head * group + part, mine] = weight.astype(BF16)

    for distance in range(1, hops):
        arrive(0, distance, 1)

    @pl.loop(0, HK)
    def _(head):
        @pl.when(head + 1 < HK)
        def _():
            for distance in range(1, hops):
                arrive(head + 1, distance, 1)

        arrive(head, hops, 1)

        for part in range(group):
            for tile in range(rows // LANES):
                mine = slice(tile * LANES, (tile + 1) * LANES)
                seen = pl.ds(tile * LANES, span)
                total = jnp.dot(weights[head * group + part, mine], vwin[head, seen], preferred_element_type=F32)
                at = pl.ds(pl.multiple_of((head * group + part) * HD, HD), HD)
                out_ref[0, mine, at] = (total / denoms[head * group + part, mine]).astype(BF16)

    for distance in range(1, hops + 1):
        @pl.when(me + distance < count)
        def _():
            seg_out(distance).wait_send()
        unsent = goes_out(distance)
        if distance == 1 and hops > 1:
            unsent = unsent & jnp.logical_not(goes_out(2))
        for which in range(2):
            for head in range(HK):
                @pl.when(unsent)
                def _():
                    block_out(which, head, distance).wait_send()
                if distance < hops:
                    @pl.when(goes_on(distance))
                    def _():
                        block_on(which, head, distance).wait_send()


def relay_kernel(
    q_ref, k_ref, v_ref, seg_ref, out_ref,
    q_own, win, segwin, krot, vturn, qrot, tops, totals, sines, cosines, bias,
    q_in, mix, mixed, lse_out, lse_in, q_sine, q_cosine, q_bias, mark, q_next, next_rot, next_bias, next_out,
    q_sem, seg_sem, own_sem, seg_send, seg_recv, back_send, back_recv, own_send, own_recv,
    near_send, near_recv, mix_send, mix_recv, lse_send, lse_recv, q_send, q_recv,
    help_send, help_recv, give_send, give_recv,
):
    me = lax.axis_index("ctx")
    count = lax.axis_size("ctx")
    rows = q_own.shape[0]
    heads = q_own.shape[1] // HD
    group = heads // HK
    scale = F32(math.log2(math.e) / math.sqrt(HD))

    def blocks(first, last):
        if isinstance(first, int):
            return pl.ds(first * LANES, (last - first) * LANES)
        return pl.ds(pl.multiple_of(first * LANES, LANES), LANES)

    def columns(head):
        return pl.ds(head * HD if isinstance(head, int) else pl.multiple_of(head * HD, HD), HD)

    def duo(pair):
        at = pair * 2 * HD
        return pl.ds(at if isinstance(pair, int) else pl.multiple_of(at, 2 * HD), 2 * HD)

    sources = (k_ref, v_ref)
    own, before, after = blocks(4, 6), blocks(2, 4), blocks(6, 8)
    own_copies = [
        pltpu.make_async_copy(sources[which].at[0], win.at[which, own], own_sem.at[which]) for which in range(2)
    ]
    seg_copy = pltpu.make_async_copy(seg_ref, segwin.at[2], seg_sem)
    q_copy = pltpu.make_async_copy(q_ref.at[0], q_own, q_sem)
    tail = pl.ds((HK - 1) * group * HD, group * HD)
    keep_copy = pltpu.make_async_copy(q_ref.at[0, :, tail], q_own.at[:, tail], q_sem)
    seg_copy.start()

    barrier = pltpu.get_barrier_semaphore()

    def greet(step, here):
        @pl.when(here)
        def _():
            pl.semaphore_signal(barrier, inc=1, device_id={"ctx": me + step})

    greet(1, me + 1 < count)
    greet(-1, me >= 1)
    greet(2, me + 2 < count)
    greet(-2, me >= 2)

    pl.semaphore_wait(barrier, jnp.minimum(me, 2) + jnp.minimum(count - 1 - me, 2))

    def remote(source, target, sent, received, there):
        return pltpu.make_async_remote_copy(
            src_ref=source, dst_ref=target, send_sem=sent, recv_sem=received, device_id={"ctx": there}
        )

    def seg_out(distance):
        return remote(
            segwin.at[2], segwin.at[2 - distance], seg_send.at[distance - 1], seg_recv.at[distance - 1], me + distance
        )

    def seg_back():
        return remote(segwin.at[2], segwin.at[1], seg_send.at[2], seg_recv.at[2], me - 1)

    def own_out(which):
        return remote(sources[which].at[0], win.at[which, before], own_send, own_recv.at[which], me + 1)

    def own_back(which):
        return remote(sources[which].at[0], win.at[which, after], back_send, back_recv.at[which], me - 1)

    helped = pl.ds(0, (HK - 1) * group * HD)

    def help_out():
        return remote(q_ref.at[0, :, helped], q_next.at[:, helped], help_send, help_recv, me - 1)

    def give_out(head):
        width = group * HD
        at = pl.ds(head * width if isinstance(head, int) else pl.multiple_of(head * width, width), width)
        return remote(next_out.at[:, at], out_ref.at[0, :, at], give_send, give_recv.at[head], me + 1)

    quarters = [(which, part) for part in range(2) for which in range(2)]

    def near_out(which, part):
        return remote(
            sources[which].at[0, blocks(1, 2), duo(part)], win.at[which, blocks(3, 4), duo(part)],
            near_send, near_recv.at[which, part], me + 1,
        )

    def near_on(which, part):
        return remote(
            win.at[which, blocks(3, 4), duo(part)], win.at[which, blocks(1, 2), duo(part)],
            near_send, near_recv.at[which, part], me + 1,
        )

    def mix_out(pair):
        return remote(mix.at[pair], mixed.at[pair], mix_send, mix_recv.at[pair], me + 1)

    def mix_on(head):
        return remote(mixed.at[head], mixed.at[head], mix_send, mix_recv.at[head], me + 1)

    few = pl.ds(0, group)

    def lse_copy(head):
        return remote(lse_out.at[head, few], lse_in.at[head, few], lse_send, lse_recv.at[head], me + 1)

    def q_back(pair):
        return remote(q_ref.at[0, blocks(0, 1), duo(pair)], q_in.at[pair], q_send, q_recv.at[pair], me - 1)

    def all_sent(ref, sent, received):
        remote(ref, ref, sent, received, me + 1).wait_send()

    freq = frequencies()
    lane = lax.broadcasted_iota(jnp.int32, (LANES, LANES), 1)
    row = lax.broadcasted_iota(jnp.int32, (LANES, LANES), 0)
    sign = jnp.where(lane < HD // 2, F32(-1.0), F32(1.0))
    ones = jnp.ones((LANES, LANES), BF16)

    def start_of(index, pieces):
        column = jnp.broadcast_to(segwin[index].astype(F32), (LANES, rows)).T
        smaller = jnp.zeros((rows, LANES), F32)
        for piece in pieces:
            smaller = smaller + jnp.where(piece < column, F32(1.0), F32(0.0))
        return jnp.dot(smaller.astype(BF16), ones, preferred_element_type=F32)

    def tables(start, block):
        sine, cosine = sin_cos(((row + block * LANES).astype(F32) - start) * freq)
        at = blocks(block, block + 1)
        sines[at] = sine * sign
        cosines[at] = cosine

    def masks(where, start, tile, low, own):
        first = start.T
        last = (lane + (own + tile) * LANES).astype(F32)
        for block in range(low, own + 1 + tile):
            key = (row + block * LANES).astype(F32)
            live = key >= first
            if block == own + tile:
                live = live & (key <= last)
            where[tile, blocks(block, block + 1)] = jnp.where(live, F32(0.0), F32(MASKED))

    def turn(head, block, keys, values):
        at = blocks(block, block + 1)
        krot[head, at] = turned(keys, cosines[at], sines[at])
        vturn[head, 0:HD, at] = values.T

    def turn_key(head, block):
        at = blocks(block, block + 1)
        turn(head, block, win[0, at, columns(head)], win[1, at, columns(head)])

    def turn_queries(head, source, target, own):
        for tile in range(2):
            place = blocks(own + tile, own + 1 + tile)
            cosine, sine = cosines[place], sines[place]
            for member in range(group):
                target[head, tile, blocks(member, member + 1)] = turned(
                    source[blocks(tile, tile + 1), columns(head * group + member)], cosine, sine
                )

    def raw_scores(keys, one):
        return lax.dot_general(keys, one, (((1,), (1,)), ((), ())), preferred_element_type=F32)

    def spread(part):
        return jnp.concatenate([part] * group, axis=1)

    def scores_of(head, tile, first, last):
        at = blocks(first, last)
        return raw_scores(krot[head, at], qrot[head, tile]) + spread(bias[tile, at])

    def summed(head, weight, at):
        return jnp.dot(vturn[head, :, at], weight.astype(BF16), preferred_element_type=F32)

    def keep(head, tile, top, both):
        tops[head, tile] = jnp.broadcast_to(top, tops.shape[2:])
        totals[head, tile] = both

    def put(head, tile, total, under, target=None):
        value = (total * (1.0 / under)).astype(BF16)
        for member in range(group):
            done = value[:, member * LANES:(member + 1) * LANES].T
            if target is None:
                out_ref[0, blocks(tile, tile + 1), columns(head * group + member)] = done
            else:
                target[blocks(tile, tile + 1), columns(head * group + member)] = done

    def fresh(head, first, last=5, ones=qrot, mask=bias):
        units = [(one, tile) for one in (head if isinstance(head, list) else [head]) for tile in range(2)]
        found = []
        for one, tile in units:
            at = blocks(first, last + tile)
            found.append(raw_scores(krot[one, at], ones[one, tile]) + spread(mask[tile, at]))
        result = []
        for (one, tile), scores in zip(units, found):
            top = jnp.max(scores, axis=0, keepdims=True)
            weight = jnp.exp2((scores - top) * scale)
            result.append((top, summed(one, weight, blocks(first, last + tile))))
        return result

    def more(head, tile, scores, first, last, extra=None):
        old = tops[head, tile, 0:1]
        top = jnp.maximum(old, jnp.max(scores, axis=0, keepdims=True))
        if extra is not None:
            top = jnp.maximum(top, extra)
        ratio = jnp.exp2((old - top) * scale)
        weight = jnp.exp2((scores - top) * scale)
        return top, totals[head, tile] * ratio + summed(head, weight, blocks(first, last))

    seg_copy.wait()
    for distance in (1, 2):
        @pl.when(me + distance < count)
        def _():
            seg_out(distance).start()

    @pl.when(me == 1)
    def _():
        seg_back().start()

    @pl.when(me == 2)
    def _():
        for pair in range(heads // 2):
            q_back(pair).start()

    @pl.when(me == 1)
    def _():
        for which, part in quarters:
            near_out(which, part).start()
        for which in range(2):
            own_back(which).start()
        help_out().start()

    @pl.when(me % 2 == 0)
    def _():
        for which in range(2):
            own_out(which).start()

    for which in range(2):
        own_copies[which].start()

    @pl.when(me == 1)
    def _():
        keep_copy.start()

    @pl.when(me != 1)
    def _():
        q_copy.start()

    @pl.when(me <= 1)
    def _():
        segwin[0] = jnp.full((1, rows), -1, jnp.int32)

    @pl.when(me == 0)
    def _():
        seg_back().wait_recv()

    for distance in (1, 2):
        @pl.when(me >= distance)
        def _():
            seg_out(distance).wait_recv()

    for which in range(2):
        own_copies[which].wait()

    pieces = []
    for index in range(3):
        seg_row = segwin[index].astype(F32)
        pieces += [seg_row[:, at:at + LANES] for at in range(0, rows, LANES)]
    shift = jnp.where(me == 0, rows, 0).astype(F32)
    begin = start_of(2, pieces) + shift
    start = start_of(1, pieces) + shift
    vturn[:, HD:] = jnp.ones((HK, vturn.shape[1] - HD, vturn.shape[2]), BF16)
    tables(begin[:LANES], 4)
    for tile in range(2):
        tables(start[tile * LANES:(tile + 1) * LANES], jnp.where(me == 0, 6, 2) + tile)

    @pl.when(me == 1)
    def _():
        late = begin[rows - 1:rows]
        sine, cosine = sin_cos(((row + 6 * LANES).astype(F32) - late) * freq)
        q_sine[...] = sine * sign
        q_cosine[...] = cosine
        for block in range(3):
            key = (row + (2 + block) * LANES).astype(F32)
            q_bias[blocks(block, block + 1)] = jnp.where(key >= late, F32(0.0), F32(MASKED))
        given = late < F32(3 * LANES)
        seen = blocks(2, 5)
        for head in range(HK):
            turn_key(head, 4)
        for which in range(2):
            own_out(which).wait_recv()

        @pl.loop(0, HK)
        def _(head):
            turn_key(head, 2)
            turn_key(head, 3)
            for part in range(group // 2):
                pair = 2 * head + part
                q_back(pair).wait_recv()
                one = jnp.concatenate(
                    [
                        turned(q_in[pair, :, member * HD:(member + 1) * HD], q_cosine[...], q_sine[...])
                        for member in range(2)
                    ],
                    axis=0,
                )
                scores = raw_scores(krot[head, seen], one) + jnp.concatenate([q_bias[...]] * 2, axis=1)
                top = jnp.max(scores, axis=0, keepdims=True)
                both = summed(head, jnp.exp2((scores - top) * scale), seen)
                under = both[HD:HD + 1]
                total = both[:HD] * (1.0 / under)
                place = blocks(4 - pair // HK, None)
                for member in range(2):
                    mix[pair, member] = jnp.where(
                        given, total[:, member * LANES:(member + 1) * LANES],
                        win[member, place, columns(pair % HK)].astype(F32),
                    ).astype(BF16)
                lse = top + jnp.log(under) * F32(math.sqrt(HD))
                for member in range(2):
                    at = 2 * part + member
                    lse_out[head, at:at + 1] = lse[:, member * LANES:(member + 1) * LANES]
                mix_out(pair).start()
            lse_copy(head).start()

    tables(begin[LANES:], 5)
    mark[...] = begin[:LANES].T[:8]
    first = jnp.where((begin < F32(LANES)) & (me == 2), F32(3 * LANES), begin)
    for tile in range(2):
        masks(bias, first[tile * LANES:(tile + 1) * LANES], tile, 0, 4)

    @pl.when(me == 1)
    def _():
        keep_copy.wait()
        head = HK - 1
        turn_queries(head, q_own, qrot, 4)
        turn_key(head, 5)
        for tile, (top, both) in enumerate(fresh(head, 2)):
            put(head, tile, both[:HD], both[HD:HD + 1])

    @pl.when(me == 0)
    def _():
        for tile in range(2):
            masks(next_bias, start[tile * LANES:(tile + 1) * LANES], tile, 4, 6)
        q_copy.wait()

        @pl.loop(0, HK)
        def _(head):
            turn_queries(head, q_own, qrot, 4)
            for block in (4, 5):
                turn_key(head, block)
            for tile, (top, both) in enumerate(fresh(head, 4)):
                put(head, tile, both[:HD], both[HD:HD + 1])

        for which in range(2):
            own_back(which).wait_recv()
        help_out().wait_recv()

        @pl.loop(0, HK - 1)
        def _(head):
            turn_queries(head, q_next, next_rot, 6)
            for block in (6, 7):
                turn_key(head, block)
            for tile, (top, both) in enumerate(fresh(head, 4, 7, next_rot, next_bias)):
                put(head, tile, both[:HD], both[HD:HD + 1], next_out)
            give_out(head).start()

    @pl.when(me >= 2)
    def _():
        start = start_of(0, pieces)
        tables(start[LANES:], 1)

        @pl.when(me == 3)
        def _():
            tables(start[:LANES], 0)

        q_copy.wait()

        @pl.loop(0, HK)
        def _(head):
            turn_queries(head, q_own, qrot, 4)
            for block in (4, 5):
                turn_key(head, block)

    @pl.when(me == 2)
    def _():
        @pl.loop(0, HK // 2)
        def _(part):
            for which in range(2):
                near_out(which, part).wait_recv()
                near_on(which, part).start()

            @pl.when(part == 1)
            def _():
                mix_out(0).wait_recv()
                mix_on(0).start()

            heads_now = [2 * part, 2 * part + 1]
            for head in heads_now:
                turn_key(head, 3)
            results = fresh(heads_now, 3)
            for at, (top, both) in enumerate(results):
                keep(heads_now[at // 2], at % 2, top, both)

        @pl.loop(0, HK // 2)
        def _(part):
            heads_now = [2 * part, 2 * part + 1]
            for head in heads_now:
                @pl.when(head > 0)
                def _():
                    mix_out(head).wait_recv()
                    mix_on(head).start()

            for head in heads_now:
                turn(head, 2, mixed[head, 0], mixed[head, 1])
            found = [scores_of(head, tile, 2, 3) for head in heads_now for tile in range(2)]
            for at, scores in enumerate(found):
                keep(heads_now[at // 2], at % 2, *more(heads_now[at // 2], at % 2, scores, 2, 3))

        @pl.loop(0, HK)
        def _(head):
            mix_out(HK + head).wait_recv()
            lse_copy(head).wait_recv()
            turn(head, 1, mixed[HK + head, 0], mixed[HK + head, 1])
            found = [scores_of(head, tile, 1, 2) for tile in range(2)]
            crossing = spread(mark[0:1] < F32(LANES))
            lse = jnp.concatenate([lse_in[head, member:member + 1] for member in range(group)], axis=1)
            lse = jnp.where(crossing, lse, F32(MASKED))
            top, both = more(head, 0, found[0], 1, 2, lse)
            share = jnp.exp2((lse - top) * scale)
            given = jnp.concatenate(
                [mixed[2 * head + member // 2, member % 2] for member in range(group)], axis=1
            )
            put(head, 0, both[:HD] + given.astype(F32) * share, both[HD:HD + 1] + share)
            top, both = more(head, 1, found[1], 1, 2)
            put(head, 1, both[:HD], both[HD:HD + 1])

    @pl.when(me == 3)
    def _():
        for which in range(2):
            own_out(which).wait_recv()

        @pl.loop(0, HK)
        def _(head):
            for block in (2, 3):
                turn_key(head, block)
            for tile, (top, both) in enumerate(fresh(head, 2)):
                keep(head, tile, top, both)

        for which, part in quarters:
            near_on(which, part).wait_recv()

        @pl.loop(0, HK)
        def _(head):
            mix_on(head).wait_recv()
            turn(head, 0, mixed[head, 0], mixed[head, 1])
            turn_key(head, 1)
            found = [scores_of(head, tile, tile, 2) for tile in range(2)]
            for tile in range(2):
                top, both = more(head, tile, found[tile], tile, 2)
                put(head, tile, both[:HD], both[HD:HD + 1])

    for distance in (1, 2):
        @pl.when(me + distance < count)
        def _():
            seg_out(distance).wait_send()

    @pl.when(me % 2 == 0)
    def _():
        all_sent(win.at[:, own], own_send, own_recv.at[0])

    @pl.when(me == 0)
    def _():
        all_sent(next_out.at[:, helped], give_send, give_recv.at[0])

    @pl.when(me == 1)
    def _():
        seg_back().wait_send()
        all_sent(win.at[:, blocks(3, 4)], near_send, near_recv.at[0, 0])
        all_sent(win.at[:, own], back_send, back_recv.at[0])
        help_out().wait_send()
        all_sent(mix, mix_send, mix_recv.at[0])
        all_sent(lse_out.at[:, few], lse_send, lse_recv.at[0])
        for head in range(HK - 1):
            give_out(head).wait_recv()

    @pl.when(me == 2)
    def _():
        all_sent(win.at[:, blocks(3, 4)], near_send, near_recv.at[0, 0])
        all_sent(mixed.at[pl.ds(0, HK)], mix_send, mix_recv.at[0])
        all_sent(q_own.at[blocks(0, 1)], q_send, q_recv.at[0])


def relay(queries, keys, values, segments):
    rows = queries.shape[1]
    heads = queries.shape[2] // HD
    width = 3 * rows
    stack = heads // HK * LANES
    anywhere = pl.BlockSpec(memory_space=pltpu.HBM)
    dma = pltpu.SemaphoreType.DMA
    return pl.pallas_call(
        relay_kernel,
        out_shape=pltpu.VMEM(queries.shape, BF16),
        in_specs=[anywhere] * 4,
        out_specs=pl.BlockSpec(memory_space=pltpu.VMEM),
        scratch_shapes=[
            pltpu.VMEM((rows, heads * HD), BF16),
            pltpu.VMEM((2, width + rows, HK * HD), BF16),
            pltpu.VMEM((3, 1, rows), jnp.int32),
            pltpu.VMEM((HK, width + rows, HD), BF16),
            pltpu.VMEM((HK, HD + 16, width + rows), BF16),
            pltpu.VMEM((HK, 2, stack, HD), BF16),
            pltpu.VMEM((HK, 2, 8, stack), F32),
            pltpu.VMEM((HK, 2, HD + 16, stack), F32),
            pltpu.VMEM((width + rows, HD), F32),
            pltpu.VMEM((width + rows, HD), F32),
            pltpu.VMEM((2, width, LANES), F32),
            pltpu.VMEM((heads // 2, LANES, 2 * HD), BF16),
            pltpu.VMEM((heads // 2, 2, LANES, HD), BF16),
            pltpu.VMEM((heads // 2, 2, LANES, HD), BF16),
            pltpu.VMEM((HK, 8, LANES), F32),
            pltpu.VMEM((HK, 8, LANES), F32),
            pltpu.VMEM((LANES, HD), F32),
            pltpu.VMEM((LANES, HD), F32),
            pltpu.VMEM((3 * LANES, LANES), F32),
            pltpu.VMEM((8, LANES), F32),
            pltpu.VMEM((rows, heads * HD), BF16),
            pltpu.VMEM((HK, 2, stack, HD), BF16),
            pltpu.VMEM((2, width + rows, LANES), F32),
            pltpu.VMEM((rows, heads * HD), BF16),
            dma, dma, dma((2,)), dma((3,)), dma((3,)), dma, dma((2,)), dma, dma((2,)),
            dma, dma((2, 2)), dma, dma((heads // 2,)), dma, dma((HK,)), dma, dma((heads // 2,)),
            dma, dma, dma, dma((HK - 1,)),
        ],
        compiler_params=pltpu.CompilerParams(
            collective_id=0, has_side_effects=True, vmem_limit_bytes=60 * 1024 * 1024
        ),
        name="attend",
    )(queries, keys, values, segments)


def body(queries, keys, values, segments):
    count = lax.axis_size("ctx")
    hops = count // 2
    rows = queries.shape[1]
    width = (hops + 1) * rows
    span = hops * rows + LANES
    heads = queries.shape[2] // HD
    if count == 4 and rows == 2 * LANES and heads == 4 * HK:
        return relay(queries, keys, values, segments)
    anywhere = pl.BlockSpec(memory_space=pltpu.HBM)
    dma = pltpu.SemaphoreType.DMA
    return pl.pallas_call(
        functools.partial(kernel, count, hops),
        out_shape=pltpu.VMEM(queries.shape, BF16),
        in_specs=[anywhere] * 4,
        out_specs=pl.BlockSpec(memory_space=pltpu.VMEM),
        scratch_shapes=[
            pltpu.VMEM((rows, heads * HD), BF16),
            pltpu.VMEM((HK, width, HD), BF16),
            pltpu.VMEM((HK, width, HD), BF16),
            pltpu.VMEM((hops + 1, 1, rows), jnp.int32),
            pltpu.VMEM((width, HD), BF16),
            pltpu.VMEM((heads, rows, HD), BF16),
            pltpu.VMEM((heads, rows, span), BF16),
            pltpu.VMEM((heads, rows, LANES), F32),
            pltpu.VMEM((hops + 1, rows, HD), F32),
            pltpu.VMEM((hops + 1, rows, HD), F32),
            pltpu.VMEM((rows // LANES, LANES, span), F32),
            dma, dma, dma((2, HK)),
            dma((hops,)), dma((hops,)),
            dma((2, HK, hops)), dma((2, HK, hops)), dma((2, HK, hops)),
        ],
        compiler_params=pltpu.CompilerParams(
            collective_id=0, has_side_effects=True, vmem_limit_bytes=60 * 1024 * 1024
        ),
        name="attend",
    )(queries, keys, values, segments)


def solution(mesh):
    placed = (P("dp", "ctx", None), P("dp", "ctx", None), P("dp", "ctx", None), P("dp", "ctx"))
    return jax.shard_map(
        body, mesh=mesh, in_specs=placed, out_specs=P("dp", "ctx", None), check_vma=False
    )
```

```python
import functools
import math

import jax
import jax.numpy as jnp
from jax import lax
from jax.experimental import pallas as pl
from jax.experimental.pallas import tpu as pltpu
from jax.sharding import PartitionSpec as P

HK = 4
HD = 128
THETA = 500000.0
LANES = 128
MASKED = -1e30
F32 = jnp.float32
BF16 = jnp.bfloat16


def sin_cos(angle):
    turns = jnp.floor(angle * (2.0 / math.pi) + 0.5)
    rest = angle - turns * 1.5703125
    rest = rest - turns * 4.837512969970703125e-4
    rest = rest - turns * 7.54978995489188216e-8
    square = rest * rest
    sine = rest + rest * square * (
        -1.6666654611e-1 + square * (8.3321608736e-3 + square * -1.9515295891e-4)
    )
    cosine = (
        1.0
        - 0.5 * square
        + square * square * (4.166664568298827e-2 + square * (-1.388731625493765e-3 + square * 2.443315711809948e-5))
    )
    quarter = turns - 4.0 * jnp.floor(turns * 0.25)
    odd = (quarter == 1.0) | (quarter == 3.0)
    sin_out = jnp.where(odd, cosine, sine)
    cos_out = jnp.where(odd, sine, cosine)
    sin_out = jnp.where(quarter >= 2.0, -sin_out, sin_out)
    cos_out = jnp.where((quarter == 1.0) | (quarter == 2.0), -cos_out, cos_out)
    return sin_out, cos_out


def frequencies():
    index = lax.broadcasted_iota(jnp.int32, (1, HD), 1) % (HD // 2)
    result = jnp.ones((1, HD), F32)
    bit = 1
    while bit < HD // 2:
        factor = math.exp(-math.log(THETA) * 2.0 * bit / HD)
        result = result * jnp.where((index // bit) % 2 == 1, F32(factor), F32(1.0))
        bit *= 2
    return result


def turned(block, cosine, sine):
    block = block.astype(F32)
    return (block * cosine + pltpu.roll(block, HD // 2, 1) * sine).astype(BF16)


def kernel(
    count, hops, q_ref, k_ref, v_ref, seg_ref, out_ref,
    q_own, kwin, vwin, segwin, krot, qrot, weights, denoms, sines, cosines, bias,
    q_sem, seg_sem, own_sem, seg_send, seg_recv, send, recv, forward,
):
    me = lax.axis_index("ctx")
    rows = q_own.shape[0]
    span = bias.shape[2]
    group = qrot.shape[0] // HK
    windows = (kwin, vwin)

    def block(which, head, distance):
        return windows[which].at[head, pl.ds((hops - distance) * rows, rows)]

    own_copies = [
        [
            pltpu.make_async_copy(
                ref.at[0, :, pl.ds(head * HD, HD)], block(which, head, 0), own_sem.at[which, head]
            )
            for head in range(HK)
        ]
        for which, ref in enumerate((k_ref, v_ref))
    ]
    seg_copy = pltpu.make_async_copy(seg_ref, segwin.at[hops], seg_sem)
    q_copy = pltpu.make_async_copy(q_ref.at[0], q_own, q_sem)
    seg_copy.start()
    for which in range(2):
        for head in range(HK):
            own_copies[which][head].start()
    q_copy.start()

    barrier = pltpu.get_barrier_semaphore()
    for distance in range(1, hops + 1):
        @pl.when(me + distance < count)
        def _():
            pl.semaphore_signal(barrier, inc=1, device_id={"ctx": me + distance})

        @pl.when(me >= distance)
        def _():
            pl.semaphore_signal(barrier, inc=1, device_id={"ctx": me - distance})
    pl.semaphore_wait(barrier, jnp.minimum(me, hops) + jnp.minimum(count - 1 - me, hops))

    def seg_out(distance):
        return pltpu.make_async_remote_copy(
            src_ref=segwin.at[hops], dst_ref=segwin.at[hops - distance],
            send_sem=seg_send.at[distance - 1], recv_sem=seg_recv.at[distance - 1],
            device_id={"ctx": me + distance},
        )

    def block_out(which, head, distance):
        return pltpu.make_async_remote_copy(
            src_ref=block(which, head, 0), dst_ref=block(which, head, distance),
            send_sem=send.at[which, head, distance - 1], recv_sem=recv.at[which, head, distance - 1],
            device_id={"ctx": me + distance},
        )

    def block_on(which, head, distance):
        return pltpu.make_async_remote_copy(
            src_ref=block(which, head, distance), dst_ref=block(which, head, distance + 1),
            send_sem=forward.at[which, head, distance - 1], recv_sem=recv.at[which, head, distance],
            device_id={"ctx": me + 1},
        )

    def goes_out(distance):
        direct = me + distance < count
        if distance > 1:
            direct = direct & ((me + distance) % 2 == 0)
        return direct

    def goes_on(distance):
        return (me % 2 == 0) & (me >= distance) & (me + 1 < count)

    seg_copy.wait()
    for distance in range(1, hops + 1):
        @pl.when(me + distance < count)
        def _():
            seg_out(distance).start()
    for which in range(2):
        for head in range(HK):
            own_copies[which][head].wait()

            @pl.when(goes_out(1))
            def _():
                block_out(which, head, 1).start()
    for distance in range(2, hops + 1):
        @pl.when(goes_out(distance))
        def _():
            for which in range(2):
                for head in range(HK):
                    if distance == 2:
                        block_out(which, head, 1).wait_send()
                    block_out(which, head, distance).start()

    for distance in range(1, hops + 1):
        @pl.when(me < distance)
        def _():
            empty = jnp.zeros((HK, rows, HD), BF16)
            kwin[:, pl.ds((hops - distance) * rows, rows)] = empty
            vwin[:, pl.ds((hops - distance) * rows, rows)] = empty
            segwin[hops - distance] = jnp.full((1, rows), -1, jnp.int32)

    for distance in range(1, hops + 1):
        @pl.when(me >= distance)
        def _():
            seg_out(distance).wait_recv()

    freq = frequencies()
    lane = lax.broadcasted_iota(jnp.int32, (rows, LANES), 1)
    row = lax.broadcasted_iota(jnp.int32, (rows, LANES), 0)
    sign = jnp.where(lane < HD // 2, F32(-1.0), F32(1.0))
    ones = jnp.ones((LANES, LANES), BF16)
    pieces = []
    for index in range(hops + 1):
        seg_row = segwin[index].astype(F32)
        pieces += [seg_row[:, at:at + LANES] for at in range(0, rows, LANES)]
    for index in range(hops + 1):
        column = jnp.broadcast_to(segwin[index].astype(F32), (LANES, rows)).T
        smaller = jnp.zeros((rows, LANES), F32)
        for piece in pieces:
            smaller = smaller + jnp.where(piece < column, F32(1.0), F32(0.0))
        start = jnp.dot(smaller.astype(BF16), ones, preferred_element_type=F32)
        position = (row + index * rows).astype(F32) - start
        sine, cosine = sin_cos(position * freq)
        sines[index] = sine * sign
        cosines[index] = cosine
        if index == hops:
            last = (row + hops * rows).astype(F32)
            for tile in range(rows // LANES):
                mine = slice(tile * LANES, (tile + 1) * LANES)
                for at in range(0, span, LANES):
                    spot = (lane[mine] + (at + tile * LANES)).astype(F32)
                    bias[tile, :, at:at + LANES] = jnp.where(
                        (spot >= start[mine]) & (spot <= last[mine]), F32(0.0), F32(MASKED)
                    )

    q_copy.wait()

    @pl.loop(0, qrot.shape[0])
    def _(head):
        at = pl.ds(pl.multiple_of(head * HD, HD), HD)
        qrot[head] = turned(q_own[:, at], cosines[hops], sines[hops])

    scale = F32(math.log2(math.e) / math.sqrt(HD))

    def arrive(head, distance, which):
        @pl.when(me >= distance)
        def _():
            block_out(which, head, distance).wait_recv()
        if distance < hops:
            @pl.when(goes_on(distance))
            def _():
                block_on(which, head, distance).start()

    @pl.loop(0, HK)
    def _(head):
        for distance in range(1, hops + 1):
            arrive(head, distance, 0)
        for index in range(hops + 1):
            at = pl.ds(index * rows, rows)
            krot[at] = turned(kwin[head, at], cosines[index], sines[index])

        for part in range(group):
            for tile in range(rows // LANES):
                mine = slice(tile * LANES, (tile + 1) * LANES)
                seen = pl.ds(tile * LANES, span)
                scores = lax.dot_general(
                    qrot[head * group + part, mine], krot[seen], (((1,), (1,)), ((), ())),
                    preferred_element_type=F32,
                ) + bias[tile]
                top = jnp.max(scores, axis=1, keepdims=True)
                weight = jnp.exp2((scores - top) * scale)
                denoms[head * group + part, mine] = jnp.broadcast_to(
                    jnp.sum(weight, axis=1, keepdims=True), (LANES, LANES)
                )
                weights[head * group + part, mine] = weight.astype(BF16)

    for distance in range(1, hops):
        arrive(0, distance, 1)

    @pl.loop(0, HK)
    def _(head):
        @pl.when(head + 1 < HK)
        def _():
            for distance in range(1, hops):
                arrive(head + 1, distance, 1)

        arrive(head, hops, 1)

        for part in range(group):
            for tile in range(rows // LANES):
                mine = slice(tile * LANES, (tile + 1) * LANES)
                seen = pl.ds(tile * LANES, span)
                total = jnp.dot(weights[head * group + part, mine], vwin[head, seen], preferred_element_type=F32)
                at = pl.ds(pl.multiple_of((head * group + part) * HD, HD), HD)
                out_ref[0, mine, at] = (total / denoms[head * group + part, mine]).astype(BF16)

    for distance in range(1, hops + 1):
        @pl.when(me + distance < count)
        def _():
            seg_out(distance).wait_send()
        unsent = goes_out(distance)
        if distance == 1 and hops > 1:
            unsent = unsent & jnp.logical_not(goes_out(2))
        for which in range(2):
            for head in range(HK):
                @pl.when(unsent)
                def _():
                    block_out(which, head, distance).wait_send()
                if distance < hops:
                    @pl.when(goes_on(distance))
                    def _():
                        block_on(which, head, distance).wait_send()


def relay_kernel(
    q_ref, k_ref, v_ref, seg_ref, out_ref,
    q_own, win, segwin, krot, vturn, qrot, tops, totals, sines, cosines, bias,
    q_in, mix, mixed, lse_out, lse_in, q_sine, q_cosine, q_bias, mark, q_next, next_rot, next_bias, next_out,
    q_sem, seg_sem, own_sem, seg_send, seg_recv, back_send, back_recv, own_send, own_recv,
    near_send, near_recv, mix_send, mix_recv, lse_send, lse_recv, q_send, q_recv,
    help_send, help_recv, give_send, give_recv,
):
    me = lax.axis_index("ctx")
    count = lax.axis_size("ctx")
    rows = q_own.shape[0]
    heads = q_own.shape[1] // HD
    group = heads // HK
    scale = F32(math.log2(math.e) / math.sqrt(HD))

    def blocks(first, last):
        if isinstance(first, int):
            return pl.ds(first * LANES, (last - first) * LANES)
        return pl.ds(pl.multiple_of(first * LANES, LANES), LANES)

    def columns(head):
        return pl.ds(head * HD if isinstance(head, int) else pl.multiple_of(head * HD, HD), HD)

    def duo(pair):
        at = pair * 2 * HD
        return pl.ds(at if isinstance(pair, int) else pl.multiple_of(at, 2 * HD), 2 * HD)

    sources = (k_ref, v_ref)
    own, before, after = blocks(4, 6), blocks(2, 4), blocks(6, 8)
    own_copies = [
        pltpu.make_async_copy(sources[which].at[0], win.at[which, own], own_sem) for which in range(2)
    ]
    seg_copy = pltpu.make_async_copy(seg_ref, segwin.at[2], seg_sem)
    q_copy = pltpu.make_async_copy(q_ref.at[0], q_own, q_sem)
    tail = pl.ds((HK - 1) * group * HD, group * HD)
    keep_copy = pltpu.make_async_copy(q_ref.at[0, :, tail], q_own.at[:, tail], q_sem)
    seg_copy.start()

    barrier = pltpu.get_barrier_semaphore()

    def greet(step, here):
        @pl.when(here)
        def _():
            pl.semaphore_signal(barrier, inc=1, device_id={"ctx": me + step})

    greet(1, me + 1 < count)
    greet(-1, me >= 1)
    greet(2, me + 2 < count)
    greet(-2, me >= 2)

    pl.semaphore_wait(barrier, jnp.minimum(me, 2) + jnp.minimum(count - 1 - me, 2))

    def remote(source, target, sent, received, there):
        return pltpu.make_async_remote_copy(
            src_ref=source, dst_ref=target, send_sem=sent, recv_sem=received, device_id={"ctx": there}
        )

    def seg_out(distance):
        return remote(
            segwin.at[2], segwin.at[2 - distance], seg_send.at[distance - 1], seg_recv.at[distance - 1], me + distance
        )

    def seg_back():
        return remote(segwin.at[2], segwin.at[1], seg_send.at[2], seg_recv.at[2], me - 1)

    def own_out(which):
        return remote(sources[which].at[0], win.at[which, before], own_send, own_recv, me + 1)

    def own_back(which):
        return remote(sources[which].at[0], win.at[which, after], back_send, back_recv, me - 1)

    helped = pl.ds(0, (HK - 1) * group * HD)

    def help_out():
        return remote(q_ref.at[0, :, helped], q_next.at[:, helped], help_send, help_recv, me - 1)

    def give_out(head):
        width = group * HD
        at = pl.ds(head * width if isinstance(head, int) else pl.multiple_of(head * width, width), width)
        return remote(next_out.at[:, at], out_ref.at[0, :, at], give_send, give_recv, me + 1)

    quarters = [(which, part) for part in range(2) for which in range(2)]

    def near_out(which, part):
        return remote(
            sources[which].at[0, blocks(1, 2), duo(part)], win.at[which, blocks(3, 4), duo(part)],
            near_send, near_recv.at[part], me + 1,
        )

    def near_on(which, part):
        return remote(
            win.at[which, blocks(3, 4), duo(part)], win.at[which, blocks(1, 2), duo(part)],
            near_send, near_recv.at[part], me + 1,
        )

    def mix_out(pair):
        return remote(mix.at[pair], mixed.at[pair], mix_send, mix_recv.at[pair], me + 1)

    def mix_on(head):
        return remote(mixed.at[head], mixed.at[head], mix_send, mix_recv.at[head], me + 1)

    few = pl.ds(0, group)

    def lse_copy(head):
        return remote(lse_out.at[head, few], lse_in.at[head, few], lse_send, lse_recv.at[head], me + 1)

    def q_back(pair):
        return remote(q_ref.at[0, blocks(0, 1), duo(pair)], q_in.at[pair], q_send, q_recv.at[pair], me - 1)

    def all_sent(ref, sent, received):
        remote(ref, ref, sent, received, me + 1).wait_send()

    def all_here(ref, sent, received):
        remote(ref, ref, sent, received, me + 1).wait_recv()

    freq = frequencies()
    lane = lax.broadcasted_iota(jnp.int32, (LANES, LANES), 1)
    row = lax.broadcasted_iota(jnp.int32, (LANES, LANES), 0)
    sign = jnp.where(lane < HD // 2, F32(-1.0), F32(1.0))
    ones = jnp.ones((LANES, LANES), BF16)

    def start_of(index, pieces):
        column = jnp.broadcast_to(segwin[index].astype(F32), (LANES, rows)).T
        smaller = jnp.zeros((rows, LANES), F32)
        for piece in pieces:
            smaller = smaller + jnp.where(piece < column, F32(1.0), F32(0.0))
        return jnp.dot(smaller.astype(BF16), ones, preferred_element_type=F32)

    def tables(start, block):
        sine, cosine = sin_cos(((row + block * LANES).astype(F32) - start) * freq)
        at = blocks(block, block + 1)
        sines[at] = sine * sign
        cosines[at] = cosine

    def masks(where, start, tile, low, own):
        first = start.T
        last = (lane + (own + tile) * LANES).astype(F32)
        for block in range(low, own + 1 + tile):
            key = (row + block * LANES).astype(F32)
            live = key >= first
            if block == own + tile:
                live = live & (key <= last)
            where[tile, blocks(block, block + 1)] = jnp.where(live, F32(0.0), F32(MASKED))

    def turn(head, block, keys, values):
        at = blocks(block, block + 1)
        krot[head, at] = turned(keys, cosines[at], sines[at])
        vturn[head, 0:HD, at] = values.T

    def place_piece(head, block, piece):
        at = blocks(block, block + 1)
        krot[head, at] = mixed[piece, 0]
        vturn[head, 0:HD, at] = mixed[piece, 1]

    def turn_key(head, block):
        at = blocks(block, block + 1)
        turn(head, block, win[0, at, columns(head)], win[1, at, columns(head)])

    def turn_queries(head, source, target, own):
        for tile in range(2):
            place = blocks(own + tile, own + 1 + tile)
            cosine, sine = cosines[place], sines[place]
            for member in range(group):
                target[head, tile, blocks(member, member + 1)] = turned(
                    source[blocks(tile, tile + 1), columns(head * group + member)], cosine, sine
                )

    def raw_scores(keys, one):
        return lax.dot_general(keys, one, (((1,), (1,)), ((), ())), preferred_element_type=F32)

    def spread(part):
        return jnp.concatenate([part] * group, axis=1)

    def scores_of(head, tile, first, last):
        at = blocks(first, last)
        return raw_scores(krot[head, at], qrot[head, tile]) + spread(bias[tile, at])

    def summed(head, weight, at):
        return jnp.dot(vturn[head, :, at], weight.astype(BF16), preferred_element_type=F32)

    def keep(head, tile, top, both):
        tops[head, tile] = jnp.broadcast_to(top, tops.shape[2:])
        totals[head, tile] = both

    def put(head, tile, total, under, target=None):
        value = (total * (1.0 / under)).astype(BF16)
        for member in range(group):
            done = value[:, member * LANES:(member + 1) * LANES].T
            if target is None:
                out_ref[0, blocks(tile, tile + 1), columns(head * group + member)] = done
            else:
                target[blocks(tile, tile + 1), columns(head * group + member)] = done

    def fresh(head, first, last=5, ones=qrot, mask=bias):
        units = [(one, tile) for one in (head if isinstance(head, list) else [head]) for tile in range(2)]
        found = []
        for one, tile in units:
            at = blocks(first, last + tile)
            found.append(raw_scores(krot[one, at], ones[one, tile]) + spread(mask[tile, at]))
        result = []
        for (one, tile), scores in zip(units, found):
            top = jnp.max(scores, axis=0, keepdims=True)
            weight = jnp.exp2((scores - top) * scale)
            result.append((top, summed(one, weight, blocks(first, last + tile))))
        return result

    def more(head, tile, scores, first, last, extra=None):
        old = tops[head, tile, 0:1]
        top = jnp.maximum(old, jnp.max(scores, axis=0, keepdims=True))
        if extra is not None:
            top = jnp.maximum(top, extra)
        ratio = jnp.exp2((old - top) * scale)
        weight = jnp.exp2((scores - top) * scale)
        return top, totals[head, tile] * ratio + summed(head, weight, blocks(first, last))

    @pl.when(me == 2)
    def _():
        for pair in range(heads // 2):
            q_back(pair).start()

    seg_copy.wait()
    for distance in (1, 2):
        @pl.when(me + distance < count)
        def _():
            seg_out(distance).start()

    @pl.when(me == 1)
    def _():
        seg_back().start()

    @pl.when(me == 1)
    def _():
        for which, part in quarters:
            near_out(which, part).start()
        for which in range(2):
            own_back(which).start()
        help_out().start()

    @pl.when(me % 2 == 0)
    def _():
        for which in range(2):
            own_out(which).start()

    for which in range(2):
        own_copies[which].start()

    @pl.when(me == 1)
    def _():
        keep_copy.start()

    @pl.when(me != 1)
    def _():
        q_copy.start()

    @pl.when(me <= 1)
    def _():
        segwin[0] = jnp.full((1, rows), -1, jnp.int32)

    @pl.when(me == 0)
    def _():
        seg_back().wait_recv()

    for distance in (1, 2):
        @pl.when(me >= distance)
        def _():
            seg_out(distance).wait_recv()

    pltpu.make_async_copy(win.at[:, own], win.at[:, own], own_sem).wait()

    pieces = []
    for index in range(3):
        seg_row = segwin[index].astype(F32)
        pieces += [seg_row[:, at:at + LANES] for at in range(0, rows, LANES)]
    shift = jnp.where(me == 0, rows, 0).astype(F32)
    begin = start_of(2, pieces) + shift
    start = start_of(1, pieces) + shift
    vturn[:, HD:] = jnp.ones((HK, vturn.shape[1] - HD, vturn.shape[2]), BF16)
    tables(begin[:LANES], 4)
    for tile in range(2):
        tables(start[tile * LANES:(tile + 1) * LANES], jnp.where(me == 0, 6, 2) + tile)

    @pl.when(me == 1)
    def _():
        late = begin[rows - 1:rows]
        sine, cosine = sin_cos(((row + 6 * LANES).astype(F32) - late) * freq)
        q_sine[...] = sine * sign
        q_cosine[...] = cosine
        for block in range(3):
            key = (row + (2 + block) * LANES).astype(F32)
            q_bias[blocks(block, block + 1)] = jnp.where(key >= late, F32(0.0), F32(MASKED))
        given = late < F32(3 * LANES)
        seen = blocks(2, 5)
        for head in range(HK):
            turn_key(head, 4)
        all_here(win.at[:, before], own_send, own_recv)

        for head in range(HK):
            turn_key(head, 2)
            turn_key(head, 3)

        @pl.loop(0, HK)
        def _(head):
            for part in range(group // 2):
                pair = 2 * head + part
                q_back(pair).wait_recv()
                one = jnp.concatenate(
                    [
                        turned(q_in[pair, :, member * HD:(member + 1) * HD], q_cosine[...], q_sine[...])
                        for member in range(2)
                    ],
                    axis=0,
                )
                scores = raw_scores(krot[head, seen], one) + jnp.concatenate([q_bias[...]] * 2, axis=1)
                top = jnp.max(scores, axis=0, keepdims=True)
                both = summed(head, jnp.exp2((scores - top) * scale), seen)
                under = both[HD:HD + 1]
                total = both[:HD] * (1.0 / under)
                place = blocks(4 - pair // HK, None)
                held = (krot[pair % HK, place], vturn[pair % HK, 0:HD, place])
                for member in range(2):
                    mix[pair, member] = jnp.where(
                        given, total[:, member * LANES:(member + 1) * LANES], held[member].astype(F32)
                    ).astype(BF16)
                lse = top + jnp.log(under) * F32(math.sqrt(HD))
                for member in range(2):
                    at = 2 * part + member
                    lse_out[head, at:at + 1] = lse[:, member * LANES:(member + 1) * LANES]
                if part == group // 2 - 1:
                    lse_copy(head).start()
                mix_out(pair).start()

    tables(begin[LANES:], 5)
    mark[...] = begin[:LANES].T[:8]
    first = jnp.where((begin < F32(LANES)) & (me == 2), F32(3 * LANES), begin)
    for tile in range(2):
        masks(bias, first[tile * LANES:(tile + 1) * LANES], tile, 0, 4)

    @pl.when(me == 1)
    def _():
        keep_copy.wait()
        head = HK - 1
        turn_queries(head, q_own, qrot, 4)
        turn_key(head, 5)
        for tile, (top, both) in enumerate(fresh(head, 2)):
            put(head, tile, both[:HD], both[HD:HD + 1])

    @pl.when(me == 0)
    def _():
        for tile in range(2):
            masks(next_bias, start[tile * LANES:(tile + 1) * LANES], tile, 4, 6)
        q_copy.wait()

        @pl.loop(0, HK)
        def _(head):
            turn_queries(head, q_own, qrot, 4)
            for block in (4, 5):
                turn_key(head, block)
            for tile, (top, both) in enumerate(fresh(head, 4)):
                put(head, tile, both[:HD], both[HD:HD + 1])

        all_here(win.at[:, after], back_send, back_recv)
        help_out().wait_recv()

        @pl.loop(0, HK - 1)
        def _(head):
            turn_queries(head, q_next, next_rot, 6)
            for block in (6, 7):
                turn_key(head, block)
            for tile, (top, both) in enumerate(fresh(head, 4, 7, next_rot, next_bias)):
                put(head, tile, both[:HD], both[HD:HD + 1], next_out)
            give_out(head).start()

    @pl.when(me >= 2)
    def _():
        @pl.when(me == 3)
        def _():
            tables(start_of(0, pieces)[LANES:], 1)

        q_copy.wait()

        @pl.loop(0, HK)
        def _(head):
            turn_queries(head, q_own, qrot, 4)
            for block in (4, 5):
                turn_key(head, block)

    @pl.when(me == 2)
    def _():
        @pl.loop(0, HK // 2)
        def _(part):
            all_here(win.at[:, blocks(3, 4), duo(part)], near_send, near_recv.at[part])
            for which in range(2):
                near_on(which, part).start()

            @pl.when(part == 1)
            def _():
                mix_out(0).wait_recv()
                mix_on(0).start()

            heads_now = [2 * part, 2 * part + 1]
            for head in heads_now:
                turn_key(head, 3)
            results = fresh(heads_now, 3)
            for at, (top, both) in enumerate(results):
                keep(heads_now[at // 2], at % 2, top, both)

        @pl.loop(0, HK // 2)
        def _(part):
            heads_now = [2 * part, 2 * part + 1]
            for head in heads_now:
                @pl.when(head > 0)
                def _():
                    mix_out(head).wait_recv()
                    mix_on(head).start()

            for head in heads_now:
                place_piece(head, 2, head)
            found = [scores_of(head, tile, 2, 3) for head in heads_now for tile in range(2)]
            for at, scores in enumerate(found):
                keep(heads_now[at // 2], at % 2, *more(heads_now[at // 2], at % 2, scores, 2, 3))

        @pl.loop(0, HK)
        def _(head):
            mix_out(HK + head).wait_recv()
            lse_copy(head).wait_recv()
            place_piece(head, 1, HK + head)
            found = [scores_of(head, tile, 1, 2) for tile in range(2)]
            crossing = spread(mark[0:1] < F32(LANES))
            lse = jnp.concatenate([lse_in[head, member:member + 1] for member in range(group)], axis=1)
            lse = jnp.where(crossing, lse, F32(MASKED))
            top, both = more(head, 0, found[0], 1, 2, lse)
            share = jnp.exp2((lse - top) * scale)
            given = jnp.concatenate(
                [mixed[2 * head + member // 2, member % 2] for member in range(group)], axis=1
            )
            put(head, 0, both[:HD] + given.astype(F32) * share, both[HD:HD + 1] + share)
            top, both = more(head, 1, found[1], 1, 2)
            put(head, 1, both[:HD], both[HD:HD + 1])

    @pl.when(me == 3)
    def _():
        all_here(win.at[:, before], own_send, own_recv)

        @pl.loop(0, HK)
        def _(head):
            for block in (2, 3):
                turn_key(head, block)
            for tile, (top, both) in enumerate(fresh(head, 2)):
                keep(head, tile, top, both)

        for part in range(2):
            all_here(win.at[:, blocks(1, 2), duo(part)], near_send, near_recv.at[part])

        @pl.loop(0, HK)
        def _(head):
            mix_on(head).wait_recv()
            place_piece(head, 0, head)
            turn_key(head, 1)
            found = [scores_of(head, tile, tile, 2) for tile in range(2)]
            for tile in range(2):
                top, both = more(head, tile, found[tile], tile, 2)
                put(head, tile, both[:HD], both[HD:HD + 1])

    for distance in (1, 2):
        @pl.when(me + distance < count)
        def _():
            seg_out(distance).wait_send()

    @pl.when(me % 2 == 0)
    def _():
        all_sent(win.at[:, own], own_send, own_recv)

    @pl.when(me == 0)
    def _():
        all_sent(next_out.at[:, helped], give_send, give_recv)

    @pl.when(me == 1)
    def _():
        seg_back().wait_send()
        all_sent(win.at[:, blocks(3, 4)], near_send, near_recv.at[0])
        all_sent(win.at[:, own], back_send, back_recv)
        help_out().wait_send()
        all_sent(mix, mix_send, mix_recv.at[0])
        all_sent(lse_out.at[:, few], lse_send, lse_recv.at[0])
        all_here(out_ref.at[0, :, helped], give_send, give_recv)

    @pl.when(me == 2)
    def _():
        all_sent(win.at[:, blocks(3, 4)], near_send, near_recv.at[0])
        all_sent(mixed.at[pl.ds(0, HK)], mix_send, mix_recv.at[0])
        all_sent(q_own.at[blocks(0, 1)], q_send, q_recv.at[0])


def relay(queries, keys, values, segments):
    rows = queries.shape[1]
    heads = queries.shape[2] // HD
    width = 3 * rows
    stack = heads // HK * LANES
    anywhere = pl.BlockSpec(memory_space=pltpu.HBM)
    dma = pltpu.SemaphoreType.DMA
    return pl.pallas_call(
        relay_kernel,
        out_shape=pltpu.VMEM(queries.shape, BF16),
        in_specs=[anywhere] * 4,
        out_specs=pl.BlockSpec(memory_space=pltpu.VMEM),
        scratch_shapes=[
            pltpu.VMEM((rows, heads * HD), BF16),
            pltpu.VMEM((2, width + rows, HK * HD), BF16),
            pltpu.VMEM((3, 1, rows), jnp.int32),
            pltpu.VMEM((HK, width + rows, HD), BF16),
            pltpu.VMEM((HK, HD + 16, width + rows), BF16),
            pltpu.VMEM((HK, 2, stack, HD), BF16),
            pltpu.VMEM((HK, 2, 8, stack), F32),
            pltpu.VMEM((HK, 2, HD + 16, stack), F32),
            pltpu.VMEM((width + rows, HD), F32),
            pltpu.VMEM((width + rows, HD), F32),
            pltpu.VMEM((2, width, LANES), F32),
            pltpu.VMEM((heads // 2, LANES, 2 * HD), BF16),
            pltpu.VMEM((heads // 2, 2, LANES, HD), BF16),
            pltpu.VMEM((heads // 2, 2, LANES, HD), BF16),
            pltpu.VMEM((HK, 8, LANES), F32),
            pltpu.VMEM((HK, 8, LANES), F32),
            pltpu.VMEM((LANES, HD), F32),
            pltpu.VMEM((LANES, HD), F32),
            pltpu.VMEM((3 * LANES, LANES), F32),
            pltpu.VMEM((8, LANES), F32),
            pltpu.VMEM((rows, heads * HD), BF16),
            pltpu.VMEM((HK, 2, stack, HD), BF16),
            pltpu.VMEM((2, width + rows, LANES), F32),
            pltpu.VMEM((rows, heads * HD), BF16),
            dma, dma, dma, dma((3,)), dma((3,)), dma, dma, dma, dma,
            dma, dma((2,)), dma, dma((heads // 2,)), dma, dma((HK,)), dma, dma((heads // 2,)),
            dma, dma, dma, dma,
        ],
        compiler_params=pltpu.CompilerParams(
            collective_id=0, has_side_effects=True, vmem_limit_bytes=60 * 1024 * 1024
        ),
        name="attend",
    )(queries, keys, values, segments)


def body(queries, keys, values, segments):
    count = lax.axis_size("ctx")
    hops = count // 2
    rows = queries.shape[1]
    width = (hops + 1) * rows
    span = hops * rows + LANES
    heads = queries.shape[2] // HD
    if count == 4 and rows == 2 * LANES and heads == 4 * HK:
        return relay(queries, keys, values, segments)
    anywhere = pl.BlockSpec(memory_space=pltpu.HBM)
    dma = pltpu.SemaphoreType.DMA
    return pl.pallas_call(
        functools.partial(kernel, count, hops),
        out_shape=pltpu.VMEM(queries.shape, BF16),
        in_specs=[anywhere] * 4,
        out_specs=pl.BlockSpec(memory_space=pltpu.VMEM),
        scratch_shapes=[
            pltpu.VMEM((rows, heads * HD), BF16),
            pltpu.VMEM((HK, width, HD), BF16),
            pltpu.VMEM((HK, width, HD), BF16),
            pltpu.VMEM((hops + 1, 1, rows), jnp.int32),
            pltpu.VMEM((width, HD), BF16),
            pltpu.VMEM((heads, rows, HD), BF16),
            pltpu.VMEM((heads, rows, span), BF16),
            pltpu.VMEM((heads, rows, LANES), F32),
            pltpu.VMEM((hops + 1, rows, HD), F32),
            pltpu.VMEM((hops + 1, rows, HD), F32),
            pltpu.VMEM((rows // LANES, LANES, span), F32),
            dma, dma, dma((2, HK)),
            dma((hops,)), dma((hops,)),
            dma((2, HK, hops)), dma((2, HK, hops)), dma((2, HK, hops)),
        ],
        compiler_params=pltpu.CompilerParams(
            collective_id=0, has_side_effects=True, vmem_limit_bytes=60 * 1024 * 1024
        ),
        name="attend",
    )(queries, keys, values, segments)


def solution(mesh):
    placed = (P("dp", "ctx", None), P("dp", "ctx", None), P("dp", "ctx", None), P("dp", "ctx"))
    return jax.shard_map(
        body, mesh=mesh, in_specs=placed, out_specs=P("dp", "ctx", None), check_vma=False
    )
```

```python
import functools
import math

import jax
import jax.numpy as jnp
from jax import lax
from jax.experimental import pallas as pl
from jax.experimental.pallas import tpu as pltpu
from jax.sharding import PartitionSpec as P

HK = 4
HD = 128
THETA = 500000.0
LANES = 128
MASKED = -1e30
F32 = jnp.float32
BF16 = jnp.bfloat16


def sin_cos(angle):
    turns = jnp.floor(angle * (2.0 / math.pi) + 0.5)
    rest = angle - turns * 1.5703125
    rest = rest - turns * 4.837512969970703125e-4
    rest = rest - turns * 7.54978995489188216e-8
    square = rest * rest
    sine = rest + rest * square * (
        -1.6666654611e-1 + square * (8.3321608736e-3 + square * -1.9515295891e-4)
    )
    cosine = (
        1.0
        - 0.5 * square
        + square * square * (4.166664568298827e-2 + square * (-1.388731625493765e-3 + square * 2.443315711809948e-5))
    )
    quarter = turns - 4.0 * jnp.floor(turns * 0.25)
    odd = (quarter == 1.0) | (quarter == 3.0)
    sin_out = jnp.where(odd, cosine, sine)
    cos_out = jnp.where(odd, sine, cosine)
    sin_out = jnp.where(quarter >= 2.0, -sin_out, sin_out)
    cos_out = jnp.where((quarter == 1.0) | (quarter == 2.0), -cos_out, cos_out)
    return sin_out, cos_out


def frequencies():
    index = lax.broadcasted_iota(jnp.int32, (1, HD), 1) % (HD // 2)
    result = jnp.ones((1, HD), F32)
    bit = 1
    while bit < HD // 2:
        factor = math.exp(-math.log(THETA) * 2.0 * bit / HD)
        result = result * jnp.where((index // bit) % 2 == 1, F32(factor), F32(1.0))
        bit *= 2
    return result


def turned(block, cosine, sine):
    block = block.astype(F32)
    return (block * cosine + pltpu.roll(block, HD // 2, 1) * sine).astype(BF16)


def kernel(
    count, hops, q_ref, k_ref, v_ref, seg_ref, out_ref,
    q_own, kwin, vwin, segwin, krot, qrot, weights, denoms, sines, cosines, bias,
    q_sem, seg_sem, own_sem, seg_send, seg_recv, send, recv, forward,
):
    me = lax.axis_index("ctx")
    rows = q_own.shape[0]
    span = bias.shape[2]
    group = qrot.shape[0] // HK
    windows = (kwin, vwin)

    def block(which, head, distance):
        return windows[which].at[head, pl.ds((hops - distance) * rows, rows)]

    own_copies = [
        [
            pltpu.make_async_copy(
                ref.at[0, :, pl.ds(head * HD, HD)], block(which, head, 0), own_sem.at[which, head]
            )
            for head in range(HK)
        ]
        for which, ref in enumerate((k_ref, v_ref))
    ]
    seg_copy = pltpu.make_async_copy(seg_ref, segwin.at[hops], seg_sem)
    q_copy = pltpu.make_async_copy(q_ref.at[0], q_own, q_sem)
    seg_copy.start()
    for which in range(2):
        for head in range(HK):
            own_copies[which][head].start()
    q_copy.start()

    barrier = pltpu.get_barrier_semaphore()
    for distance in range(1, hops + 1):
        @pl.when(me + distance < count)
        def _():
            pl.semaphore_signal(barrier, inc=1, device_id={"ctx": me + distance})

        @pl.when(me >= distance)
        def _():
            pl.semaphore_signal(barrier, inc=1, device_id={"ctx": me - distance})
    pl.semaphore_wait(barrier, jnp.minimum(me, hops) + jnp.minimum(count - 1 - me, hops))

    def seg_out(distance):
        return pltpu.make_async_remote_copy(
            src_ref=segwin.at[hops], dst_ref=segwin.at[hops - distance],
            send_sem=seg_send.at[distance - 1], recv_sem=seg_recv.at[distance - 1],
            device_id={"ctx": me + distance},
        )

    def block_out(which, head, distance):
        return pltpu.make_async_remote_copy(
            src_ref=block(which, head, 0), dst_ref=block(which, head, distance),
            send_sem=send.at[which, head, distance - 1], recv_sem=recv.at[which, head, distance - 1],
            device_id={"ctx": me + distance},
        )

    def block_on(which, head, distance):
        return pltpu.make_async_remote_copy(
            src_ref=block(which, head, distance), dst_ref=block(which, head, distance + 1),
            send_sem=forward.at[which, head, distance - 1], recv_sem=recv.at[which, head, distance],
            device_id={"ctx": me + 1},
        )

    def goes_out(distance):
        direct = me + distance < count
        if distance > 1:
            direct = direct & ((me + distance) % 2 == 0)
        return direct

    def goes_on(distance):
        return (me % 2 == 0) & (me >= distance) & (me + 1 < count)

    seg_copy.wait()
    for distance in range(1, hops + 1):
        @pl.when(me + distance < count)
        def _():
            seg_out(distance).start()
    for which in range(2):
        for head in range(HK):
            own_copies[which][head].wait()

            @pl.when(goes_out(1))
            def _():
                block_out(which, head, 1).start()
    for distance in range(2, hops + 1):
        @pl.when(goes_out(distance))
        def _():
            for which in range(2):
                for head in range(HK):
                    if distance == 2:
                        block_out(which, head, 1).wait_send()
                    block_out(which, head, distance).start()

    for distance in range(1, hops + 1):
        @pl.when(me < distance)
        def _():
            empty = jnp.zeros((HK, rows, HD), BF16)
            kwin[:, pl.ds((hops - distance) * rows, rows)] = empty
            vwin[:, pl.ds((hops - distance) * rows, rows)] = empty
            segwin[hops - distance] = jnp.full((1, rows), -1, jnp.int32)

    for distance in range(1, hops + 1):
        @pl.when(me >= distance)
        def _():
            seg_out(distance).wait_recv()

    freq = frequencies()
    lane = lax.broadcasted_iota(jnp.int32, (rows, LANES), 1)
    row = lax.broadcasted_iota(jnp.int32, (rows, LANES), 0)
    sign = jnp.where(lane < HD // 2, F32(-1.0), F32(1.0))
    ones = jnp.ones((LANES, LANES), BF16)
    pieces = []
    for index in range(hops + 1):
        seg_row = segwin[index].astype(F32)
        pieces += [seg_row[:, at:at + LANES] for at in range(0, rows, LANES)]
    for index in range(hops + 1):
        column = jnp.broadcast_to(segwin[index].astype(F32), (LANES, rows)).T
        smaller = jnp.zeros((rows, LANES), F32)
        for piece in pieces:
            smaller = smaller + jnp.where(piece < column, F32(1.0), F32(0.0))
        start = jnp.dot(smaller.astype(BF16), ones, preferred_element_type=F32)
        position = (row + index * rows).astype(F32) - start
        sine, cosine = sin_cos(position * freq)
        sines[index] = sine * sign
        cosines[index] = cosine
        if index == hops:
            last = (row + hops * rows).astype(F32)
            for tile in range(rows // LANES):
                mine = slice(tile * LANES, (tile + 1) * LANES)
                for at in range(0, span, LANES):
                    spot = (lane[mine] + (at + tile * LANES)).astype(F32)
                    bias[tile, :, at:at + LANES] = jnp.where(
                        (spot >= start[mine]) & (spot <= last[mine]), F32(0.0), F32(MASKED)
                    )

    q_copy.wait()

    @pl.loop(0, qrot.shape[0])
    def _(head):
        at = pl.ds(pl.multiple_of(head * HD, HD), HD)
        qrot[head] = turned(q_own[:, at], cosines[hops], sines[hops])

    scale = F32(math.log2(math.e) / math.sqrt(HD))

    def arrive(head, distance, which):
        @pl.when(me >= distance)
        def _():
            block_out(which, head, distance).wait_recv()
        if distance < hops:
            @pl.when(goes_on(distance))
            def _():
                block_on(which, head, distance).start()

    @pl.loop(0, HK)
    def _(head):
        for distance in range(1, hops + 1):
            arrive(head, distance, 0)
        for index in range(hops + 1):
            at = pl.ds(index * rows, rows)
            krot[at] = turned(kwin[head, at], cosines[index], sines[index])

        for part in range(group):
            for tile in range(rows // LANES):
                mine = slice(tile * LANES, (tile + 1) * LANES)
                seen = pl.ds(tile * LANES, span)
                scores = lax.dot_general(
                    qrot[head * group + part, mine], krot[seen], (((1,), (1,)), ((), ())),
                    preferred_element_type=F32,
                ) + bias[tile]
                top = jnp.max(scores, axis=1, keepdims=True)
                weight = jnp.exp2((scores - top) * scale)
                denoms[head * group + part, mine] = jnp.broadcast_to(
                    jnp.sum(weight, axis=1, keepdims=True), (LANES, LANES)
                )
                weights[head * group + part, mine] = weight.astype(BF16)

    for distance in range(1, hops):
        arrive(0, distance, 1)

    @pl.loop(0, HK)
    def _(head):
        @pl.when(head + 1 < HK)
        def _():
            for distance in range(1, hops):
                arrive(head + 1, distance, 1)

        arrive(head, hops, 1)

        for part in range(group):
            for tile in range(rows // LANES):
                mine = slice(tile * LANES, (tile + 1) * LANES)
                seen = pl.ds(tile * LANES, span)
                total = jnp.dot(weights[head * group + part, mine], vwin[head, seen], preferred_element_type=F32)
                at = pl.ds(pl.multiple_of((head * group + part) * HD, HD), HD)
                out_ref[0, mine, at] = (total / denoms[head * group + part, mine]).astype(BF16)

    for distance in range(1, hops + 1):
        @pl.when(me + distance < count)
        def _():
            seg_out(distance).wait_send()
        unsent = goes_out(distance)
        if distance == 1 and hops > 1:
            unsent = unsent & jnp.logical_not(goes_out(2))
        for which in range(2):
            for head in range(HK):
                @pl.when(unsent)
                def _():
                    block_out(which, head, distance).wait_send()
                if distance < hops:
                    @pl.when(goes_on(distance))
                    def _():
                        block_on(which, head, distance).wait_send()


def relay_kernel(
    q_ref, k_ref, v_ref, seg_ref, out_ref,
    q_own, win, segwin, krot, vturn, qrot, tops, totals, sines, cosines, bias,
    q_in, mix, mixed, lse_out, lse_in, q_sine, q_cosine, q_bias, mark, q_next, next_rot, next_bias, next_out,
    q_sem, seg_sem, own_sem, seg_send, seg_recv, back_send, back_recv, own_send, own_recv,
    near_send, near_recv, mix_send, mix_recv, lse_send, lse_recv, q_send, q_recv,
    help_send, help_recv, give_send, give_recv,
):
    me = lax.axis_index("ctx")
    count = lax.axis_size("ctx")
    rows = q_own.shape[0]
    heads = q_own.shape[1] // HD
    group = heads // HK
    scale = F32(math.log2(math.e) / math.sqrt(HD))

    def blocks(first, last):
        if isinstance(first, int):
            return pl.ds(first * LANES, (last - first) * LANES)
        return pl.ds(pl.multiple_of(first * LANES, LANES), LANES)

    def columns(head):
        return pl.ds(head * HD if isinstance(head, int) else pl.multiple_of(head * HD, HD), HD)

    def duo(pair):
        at = pair * 2 * HD
        return pl.ds(at if isinstance(pair, int) else pl.multiple_of(at, 2 * HD), 2 * HD)

    sources = (k_ref, v_ref)
    own, before, after = blocks(4, 6), blocks(2, 4), blocks(6, 8)
    own_copies = [
        pltpu.make_async_copy(sources[which].at[0], win.at[which, own], own_sem) for which in range(2)
    ]
    seg_copy = pltpu.make_async_copy(seg_ref, segwin.at[2], seg_sem)
    q_copy = pltpu.make_async_copy(q_ref.at[0], q_own, q_sem)
    tail = pl.ds((HK - 1) * group * HD, group * HD)
    keep_copy = pltpu.make_async_copy(q_ref.at[0, :, tail], q_own.at[:, tail], q_sem)
    seg_copy.start()

    barrier = pltpu.get_barrier_semaphore()

    def greet(step, here):
        @pl.when(here)
        def _():
            pl.semaphore_signal(barrier, inc=1, device_id={"ctx": me + step})

    greet(1, me + 1 < count)
    greet(-1, me >= 1)
    greet(2, me + 2 < count)
    greet(-2, me >= 2)

    pl.semaphore_wait(barrier, jnp.minimum(me, 2) + jnp.minimum(count - 1 - me, 2))

    def remote(source, target, sent, received, there):
        return pltpu.make_async_remote_copy(
            src_ref=source, dst_ref=target, send_sem=sent, recv_sem=received, device_id={"ctx": there}
        )

    def seg_out(distance):
        return remote(
            segwin.at[2], segwin.at[2 - distance], seg_send.at[distance - 1], seg_recv.at[distance - 1], me + distance
        )

    def seg_back():
        return remote(segwin.at[2], segwin.at[1], seg_send.at[2], seg_recv.at[2], me - 1)

    def own_out(which):
        return remote(sources[which].at[0], win.at[which, before], own_send, own_recv, me + 1)

    def own_back(which):
        return remote(sources[which].at[0], win.at[which, after], back_send, back_recv, me - 1)

    helped = pl.ds(0, (HK - 1) * group * HD)

    def help_out():
        return remote(q_ref.at[0, :, helped], q_next.at[:, helped], help_send, help_recv, me - 1)

    def give_out(head):
        width = group * HD
        at = pl.ds(head * width if isinstance(head, int) else pl.multiple_of(head * width, width), width)
        return remote(next_out.at[:, at], out_ref.at[0, :, at], give_send, give_recv, me + 1)

    quarters = [(which, part) for part in range(2) for which in range(2)]

    def near_out(which, part):
        return remote(
            sources[which].at[0, blocks(1, 2), duo(part)], win.at[which, blocks(3, 4), duo(part)],
            near_send, near_recv.at[part], me + 1,
        )

    def near_on(which, part):
        return remote(
            win.at[which, blocks(3, 4), duo(part)], win.at[which, blocks(1, 2), duo(part)],
            near_send, near_recv.at[part], me + 1,
        )

    def mix_out(pair):
        return remote(mix.at[pair], mixed.at[pair], mix_send, mix_recv.at[pair], me + 1)

    def mix_on(head):
        return remote(mixed.at[head], mixed.at[head], mix_send, mix_recv.at[head], me + 1)

    few = pl.ds(0, group)

    def lse_copy(head):
        return remote(lse_out.at[head, few], lse_in.at[head, few], lse_send, lse_recv.at[head], me + 1)

    def q_back(pair):
        return remote(q_ref.at[0, blocks(0, 1), duo(pair)], q_in.at[pair], q_send, q_recv.at[pair], me - 1)

    final = heads // 2 - 1

    def q_half(member):
        return remote(
            q_ref.at[0, blocks(0, 1), columns(2 * final + member)], q_in.at[final, :, columns(member)],
            q_send, q_recv.at[final + member], me - 1,
        )

    def mix_half(member):
        return remote(mix.at[final, member], mixed.at[final, member], mix_send, mix_recv.at[final], me + 1)

    def all_sent(ref, sent, received):
        remote(ref, ref, sent, received, me + 1).wait_send()

    def all_here(ref, sent, received):
        remote(ref, ref, sent, received, me + 1).wait_recv()

    freq = frequencies()
    lane = lax.broadcasted_iota(jnp.int32, (LANES, LANES), 1)
    row = lax.broadcasted_iota(jnp.int32, (LANES, LANES), 0)
    sign = jnp.where(lane < HD // 2, F32(-1.0), F32(1.0))
    ones = jnp.ones((LANES, LANES), BF16)

    def start_of(index, pieces):
        column = jnp.broadcast_to(segwin[index].astype(F32), (LANES, rows)).T
        smaller = jnp.zeros((rows, LANES), F32)
        for piece in pieces:
            smaller = smaller + jnp.where(piece < column, F32(1.0), F32(0.0))
        return jnp.dot(smaller.astype(BF16), ones, preferred_element_type=F32)

    def tables(start, block):
        sine, cosine = sin_cos(((row + block * LANES).astype(F32) - start) * freq)
        at = blocks(block, block + 1)
        sines[at] = sine * sign
        cosines[at] = cosine

    def masks(where, start, tile, low, own):
        first = start.T
        last = (lane + (own + tile) * LANES).astype(F32)
        for block in range(low, own + 1 + tile):
            key = (row + block * LANES).astype(F32)
            live = key >= first
            if block == own + tile:
                live = live & (key <= last)
            where[tile, blocks(block, block + 1)] = jnp.where(live, F32(0.0), F32(MASKED))

    def turn(head, block, keys, values):
        at = blocks(block, block + 1)
        krot[head, at] = turned(keys, cosines[at], sines[at])
        vturn[head, 0:HD, at] = values.T

    def place_piece(head, block, piece):
        at = blocks(block, block + 1)
        krot[head, at] = mixed[piece, 0]
        vturn[head, 0:HD, at] = mixed[piece, 1]

    def turn_key(head, block):
        at = blocks(block, block + 1)
        turn(head, block, win[0, at, columns(head)], win[1, at, columns(head)])

    def turn_queries(head, source, target, own):
        for tile in range(2):
            place = blocks(own + tile, own + 1 + tile)
            cosine, sine = cosines[place], sines[place]
            for member in range(group):
                target[head, tile, blocks(member, member + 1)] = turned(
                    source[blocks(tile, tile + 1), columns(head * group + member)], cosine, sine
                )

    def raw_scores(keys, one):
        return lax.dot_general(keys, one, (((1,), (1,)), ((), ())), preferred_element_type=F32)

    def spread(part):
        return jnp.concatenate([part] * group, axis=1)

    def scores_of(head, tile, first, last):
        at = blocks(first, last)
        return raw_scores(krot[head, at], qrot[head, tile]) + spread(bias[tile, at])

    def summed(head, weight, at):
        return jnp.dot(vturn[head, :, at], weight.astype(BF16), preferred_element_type=F32)

    def keep(head, tile, top, both):
        tops[head, tile] = jnp.broadcast_to(top, tops.shape[2:])
        totals[head, tile] = both

    def put(head, tile, total, under, target=None):
        value = (total * (1.0 / under)).astype(BF16)
        for member in range(group):
            done = value[:, member * LANES:(member + 1) * LANES].T
            if target is None:
                out_ref[0, blocks(tile, tile + 1), columns(head * group + member)] = done
            else:
                target[blocks(tile, tile + 1), columns(head * group + member)] = done

    def fresh(head, first, last=5, ones=qrot, mask=bias):
        units = [(one, tile) for one in (head if isinstance(head, list) else [head]) for tile in range(2)]
        found = []
        for one, tile in units:
            at = blocks(first, last + tile)
            found.append(raw_scores(krot[one, at], ones[one, tile]) + spread(mask[tile, at]))
        result = []
        for (one, tile), scores in zip(units, found):
            top = jnp.max(scores, axis=0, keepdims=True)
            weight = jnp.exp2((scores - top) * scale)
            result.append((top, summed(one, weight, blocks(first, last + tile))))
        return result

    def more(head, tile, scores, first, last, extra=None):
        old = tops[head, tile, 0:1]
        top = jnp.maximum(old, jnp.max(scores, axis=0, keepdims=True))
        if extra is not None:
            top = jnp.maximum(top, extra)
        ratio = jnp.exp2((old - top) * scale)
        weight = jnp.exp2((scores - top) * scale)
        return top, totals[head, tile] * ratio + summed(head, weight, blocks(first, last))

    @pl.when(me == 2)
    def _():
        for pair in range(heads // 2 - 1):
            q_back(pair).start()
        for member in range(2):
            q_half(member).start()

    seg_copy.wait()
    for distance in (1, 2):
        @pl.when(me + distance < count)
        def _():
            seg_out(distance).start()

    @pl.when(me == 1)
    def _():
        seg_back().start()

    @pl.when(me == 1)
    def _():
        for which, part in quarters:
            near_out(which, part).start()
        for which in range(2):
            own_back(which).start()
        help_out().start()

    @pl.when(me % 2 == 0)
    def _():
        for which in range(2):
            own_out(which).start()

    for which in range(2):
        own_copies[which].start()

    @pl.when(me == 1)
    def _():
        keep_copy.start()

    @pl.when(me != 1)
    def _():
        q_copy.start()

    @pl.when(me <= 1)
    def _():
        segwin[0] = jnp.full((1, rows), -1, jnp.int32)

    @pl.when(me == 0)
    def _():
        seg_back().wait_recv()

    for distance in (1, 2):
        @pl.when(me >= distance)
        def _():
            seg_out(distance).wait_recv()

    pltpu.make_async_copy(win.at[:, own], win.at[:, own], own_sem).wait()

    pieces = []
    for index in range(3):
        seg_row = segwin[index].astype(F32)
        pieces += [seg_row[:, at:at + LANES] for at in range(0, rows, LANES)]
    shift = jnp.where(me == 0, rows, 0).astype(F32)
    begin = start_of(2, pieces) + shift
    start = start_of(1, pieces) + shift
    vturn[:, HD:] = jnp.ones((HK, vturn.shape[1] - HD, vturn.shape[2]), BF16)
    tables(begin[:LANES], 4)
    for tile in range(2):
        tables(start[tile * LANES:(tile + 1) * LANES], jnp.where(me == 0, 6, 2) + tile)

    @pl.when(me == 1)
    def _():
        late = begin[rows - 1:rows]
        sine, cosine = sin_cos(((row + 6 * LANES).astype(F32) - late) * freq)
        q_sine[...] = sine * sign
        q_cosine[...] = cosine
        for block in range(3):
            key = (row + (2 + block) * LANES).astype(F32)
            q_bias[blocks(block, block + 1)] = jnp.where(key >= late, F32(0.0), F32(MASKED))
        given = late < F32(3 * LANES)
        seen = blocks(2, 5)
        for head in range(HK):
            turn_key(head, 4)
        all_here(win.at[:, before], own_send, own_recv)

        for head in range(HK):
            turn_key(head, 2)
            turn_key(head, 3)

        def serve(head, part, members):
            pair = 2 * head + part
            turns = [
                turned(q_in[pair, :, member * HD:(member + 1) * HD], q_cosine[...], q_sine[...]) for member in members
            ]
            scores = raw_scores(krot[head, seen], jnp.concatenate(turns, axis=0))
            scores = scores + jnp.concatenate([q_bias[...]] * len(members), axis=1)
            top = jnp.max(scores, axis=0, keepdims=True)
            both = summed(head, jnp.exp2((scores - top) * scale), seen)
            under = both[HD:HD + 1]
            total = both[:HD] * (1.0 / under)
            place = blocks(4 - pair // HK, None) if not isinstance(pair, int) else blocks(4 - pair // HK, 5 - pair // HK)
            held = (krot[pair % HK, place], vturn[pair % HK, 0:HD, place])
            lse = top + jnp.log(under) * F32(math.sqrt(HD))
            for index, member in enumerate(members):
                mine = slice(index * LANES, (index + 1) * LANES)
                mix[pair, member] = jnp.where(given, total[:, mine], held[member].astype(F32)).astype(BF16)
                at = 2 * part + member
                lse_out[head, at:at + 1] = lse[:, mine]

        @pl.loop(0, HK - 1)
        def _(head):
            for part in range(group // 2):
                q_back(2 * head + part).wait_recv()
                serve(head, part, [0, 1])
                if part == group // 2 - 1:
                    lse_copy(head).start()
                mix_out(2 * head + part).start()

        q_back(heads // 2 - 2).wait_recv()
        serve(HK - 1, 0, [0, 1])
        mix_out(heads // 2 - 2).start()
        for member in range(2):
            q_half(member).wait_recv()
            serve(HK - 1, 1, [member])
            if member == 1:
                lse_copy(HK - 1).start()
            mix_half(member).start()

    tables(begin[LANES:], 5)
    mark[...] = begin[:LANES].T[:8]
    first = jnp.where((begin < F32(LANES)) & (me == 2), F32(3 * LANES), begin)
    for tile in range(2):
        masks(bias, first[tile * LANES:(tile + 1) * LANES], tile, 0, 4)

    @pl.when(me == 1)
    def _():
        keep_copy.wait()
        head = HK - 1
        turn_queries(head, q_own, qrot, 4)
        turn_key(head, 5)
        for tile, (top, both) in enumerate(fresh(head, 2)):
            put(head, tile, both[:HD], both[HD:HD + 1])

    @pl.when(me == 0)
    def _():
        for tile in range(2):
            masks(next_bias, start[tile * LANES:(tile + 1) * LANES], tile, 4, 6)
        q_copy.wait()

        @pl.loop(0, HK)
        def _(head):
            turn_queries(head, q_own, qrot, 4)
            for block in (4, 5):
                turn_key(head, block)
            for tile, (top, both) in enumerate(fresh(head, 4)):
                put(head, tile, both[:HD], both[HD:HD + 1])

        all_here(win.at[:, after], back_send, back_recv)
        help_out().wait_recv()

        @pl.loop(0, HK - 1)
        def _(head):
            turn_queries(head, q_next, next_rot, 6)
            for block in (6, 7):
                turn_key(head, block)
            for tile, (top, both) in enumerate(fresh(head, 4, 7, next_rot, next_bias)):
                put(head, tile, both[:HD], both[HD:HD + 1], next_out)
            give_out(head).start()

    @pl.when(me >= 2)
    def _():
        @pl.when(me == 3)
        def _():
            tables(start_of(0, pieces)[LANES:], 1)

        q_copy.wait()

        @pl.loop(0, HK)
        def _(head):
            turn_queries(head, q_own, qrot, 4)
            for block in (4, 5):
                turn_key(head, block)

    @pl.when(me == 2)
    def _():
        @pl.loop(0, HK // 2)
        def _(part):
            all_here(win.at[:, blocks(3, 4), duo(part)], near_send, near_recv.at[part])
            for which in range(2):
                near_on(which, part).start()

            @pl.when(part == 1)
            def _():
                mix_out(0).wait_recv()
                mix_on(0).start()

            heads_now = [2 * part, 2 * part + 1]
            for head in heads_now:
                turn_key(head, 3)
            results = fresh(heads_now, 3)
            for at, (top, both) in enumerate(results):
                keep(heads_now[at // 2], at % 2, top, both)

        @pl.loop(0, HK // 2)
        def _(part):
            heads_now = [2 * part, 2 * part + 1]
            for head in heads_now:
                @pl.when(head > 0)
                def _():
                    mix_out(head).wait_recv()
                    mix_on(head).start()

            for head in heads_now:
                place_piece(head, 2, head)
            found = [scores_of(head, tile, 2, 3) for head in heads_now for tile in range(2)]
            for at, scores in enumerate(found):
                keep(heads_now[at // 2], at % 2, *more(heads_now[at // 2], at % 2, scores, 2, 3))

        @pl.loop(0, HK)
        def _(head):
            mix_out(HK + head).wait_recv()
            lse_copy(head).wait_recv()
            place_piece(head, 1, HK + head)
            found = [scores_of(head, tile, 1, 2) for tile in range(2)]
            crossing = spread(mark[0:1] < F32(LANES))
            lse = jnp.concatenate([lse_in[head, member:member + 1] for member in range(group)], axis=1)
            lse = jnp.where(crossing, lse, F32(MASKED))
            top, both = more(head, 0, found[0], 1, 2, lse)
            share = jnp.exp2((lse - top) * scale)
            given = jnp.concatenate(
                [mixed[2 * head + member // 2, member % 2] for member in range(group)], axis=1
            )
            put(head, 0, both[:HD] + given.astype(F32) * share, both[HD:HD + 1] + share)
            top, both = more(head, 1, found[1], 1, 2)
            put(head, 1, both[:HD], both[HD:HD + 1])

    @pl.when(me == 3)
    def _():
        all_here(win.at[:, before], own_send, own_recv)

        @pl.loop(0, HK)
        def _(head):
            for block in (2, 3):
                turn_key(head, block)
            for tile, (top, both) in enumerate(fresh(head, 2)):
                keep(head, tile, top, both)

        for part in range(2):
            all_here(win.at[:, blocks(1, 2), duo(part)], near_send, near_recv.at[part])

        @pl.loop(0, HK)
        def _(head):
            mix_on(head).wait_recv()
            place_piece(head, 0, head)
            turn_key(head, 1)
            found = [scores_of(head, tile, tile, 2) for tile in range(2)]
            for tile in range(2):
                top, both = more(head, tile, found[tile], tile, 2)
                put(head, tile, both[:HD], both[HD:HD + 1])

    for distance in (1, 2):
        @pl.when(me + distance < count)
        def _():
            seg_out(distance).wait_send()

    @pl.when(me % 2 == 0)
    def _():
        all_sent(win.at[:, own], own_send, own_recv)

    @pl.when(me == 0)
    def _():
        all_sent(next_out.at[:, helped], give_send, give_recv)

    @pl.when(me == 1)
    def _():
        seg_back().wait_send()
        all_sent(win.at[:, blocks(3, 4)], near_send, near_recv.at[0])
        all_sent(win.at[:, own], back_send, back_recv)
        help_out().wait_send()
        all_sent(mix, mix_send, mix_recv.at[0])
        all_sent(lse_out.at[:, few], lse_send, lse_recv.at[0])
        all_here(out_ref.at[0, :, helped], give_send, give_recv)

    @pl.when(me == 2)
    def _():
        all_sent(win.at[:, blocks(3, 4)], near_send, near_recv.at[0])
        all_sent(mixed.at[pl.ds(0, HK)], mix_send, mix_recv.at[0])
        all_sent(q_own.at[blocks(0, 1)], q_send, q_recv.at[0])


def relay(queries, keys, values, segments):
    rows = queries.shape[1]
    heads = queries.shape[2] // HD
    width = 3 * rows
    stack = heads // HK * LANES
    anywhere = pl.BlockSpec(memory_space=pltpu.HBM)
    dma = pltpu.SemaphoreType.DMA
    return pl.pallas_call(
        relay_kernel,
        out_shape=pltpu.VMEM(queries.shape, BF16),
        in_specs=[anywhere] * 4,
        out_specs=pl.BlockSpec(memory_space=pltpu.VMEM),
        scratch_shapes=[
            pltpu.VMEM((rows, heads * HD), BF16),
            pltpu.VMEM((2, width + rows, HK * HD), BF16),
            pltpu.VMEM((3, 1, rows), jnp.int32),
            pltpu.VMEM((HK, width + rows, HD), BF16),
            pltpu.VMEM((HK, HD + 16, width + rows), BF16),
            pltpu.VMEM((HK, 2, stack, HD), BF16),
            pltpu.VMEM((HK, 2, 8, stack), F32),
            pltpu.VMEM((HK, 2, HD + 16, stack), F32),
            pltpu.VMEM((width + rows, HD), F32),
            pltpu.VMEM((width + rows, HD), F32),
            pltpu.VMEM((2, width, LANES), F32),
            pltpu.VMEM((heads // 2, LANES, 2 * HD), BF16),
            pltpu.VMEM((heads // 2, 2, LANES, HD), BF16),
            pltpu.VMEM((heads // 2, 2, LANES, HD), BF16),
            pltpu.VMEM((HK, 8, LANES), F32),
            pltpu.VMEM((HK, 8, LANES), F32),
            pltpu.VMEM((LANES, HD), F32),
            pltpu.VMEM((LANES, HD), F32),
            pltpu.VMEM((3 * LANES, LANES), F32),
            pltpu.VMEM((8, LANES), F32),
            pltpu.VMEM((rows, heads * HD), BF16),
            pltpu.VMEM((HK, 2, stack, HD), BF16),
            pltpu.VMEM((2, width + rows, LANES), F32),
            pltpu.VMEM((rows, heads * HD), BF16),
            dma, dma, dma, dma((3,)), dma((3,)), dma, dma, dma, dma,
            dma, dma((2,)), dma, dma((heads // 2,)), dma, dma((HK,)), dma, dma((heads // 2 + 1,)),
            dma, dma, dma, dma,
        ],
        compiler_params=pltpu.CompilerParams(
            collective_id=0, has_side_effects=True, vmem_limit_bytes=60 * 1024 * 1024
        ),
        name="attend",
    )(queries, keys, values, segments)


def body(queries, keys, values, segments):
    count = lax.axis_size("ctx")
    hops = count // 2
    rows = queries.shape[1]
    width = (hops + 1) * rows
    span = hops * rows + LANES
    heads = queries.shape[2] // HD
    if count == 4 and rows == 2 * LANES and heads == 4 * HK:
        return relay(queries, keys, values, segments)
    anywhere = pl.BlockSpec(memory_space=pltpu.HBM)
    dma = pltpu.SemaphoreType.DMA
    return pl.pallas_call(
        functools.partial(kernel, count, hops),
        out_shape=pltpu.VMEM(queries.shape, BF16),
        in_specs=[anywhere] * 4,
        out_specs=pl.BlockSpec(memory_space=pltpu.VMEM),
        scratch_shapes=[
            pltpu.VMEM((rows, heads * HD), BF16),
            pltpu.VMEM((HK, width, HD), BF16),
            pltpu.VMEM((HK, width, HD), BF16),
            pltpu.VMEM((hops + 1, 1, rows), jnp.int32),
            pltpu.VMEM((width, HD), BF16),
            pltpu.VMEM((heads, rows, HD), BF16),
            pltpu.VMEM((heads, rows, span), BF16),
            pltpu.VMEM((heads, rows, LANES), F32),
            pltpu.VMEM((hops + 1, rows, HD), F32),
            pltpu.VMEM((hops + 1, rows, HD), F32),
            pltpu.VMEM((rows // LANES, LANES, span), F32),
            dma, dma, dma((2, HK)),
            dma((hops,)), dma((hops,)),
            dma((2, HK, hops)), dma((2, HK, hops)), dma((2, HK, hops)),
        ],
        compiler_params=pltpu.CompilerParams(
            collective_id=0, has_side_effects=True, vmem_limit_bytes=60 * 1024 * 1024
        ),
        name="attend",
    )(queries, keys, values, segments)


def solution(mesh):
    placed = (P("dp", "ctx", None), P("dp", "ctx", None), P("dp", "ctx", None), P("dp", "ctx"))
    return jax.shard_map(
        body, mesh=mesh, in_specs=placed, out_specs=P("dp", "ctx", None), check_vma=False
    )
```
